128 devices in a mesh: row: 8 (over z, core), col: 16 (over y, x).
Axes of the slice: x: 4, y: 4, z: 4, core: 2. Of those that a mesh axis runs over, the one named last changes fastest.
Arguments:
- tiles: float32 [8, 192, 3, 256, 256], P('row', 'col'), may hold values from 0.02 to 1
- slot_tile: int32 [8, 192], P('row', 'col'), may hold values from -1 to 15, as said below
Outputs:
- level_one: float32 [4, 4096, 8192], P(None, 'row', 'col')
- level_two: float32 [4, 2048, 4096], P(None, 'row', 'col')
- level_three: float32 [4, 1024, 2048], P(None, 'row', 'col')
The draws below stay inside these ranges and needn't reach their ends.
Inputs may be any that keep to these rules, and one draw needn't show every extreme that they name: Slot s of device (i, j) is slot_tile[i, j * 12 + s]. A live slot holds the position p of its tile within the device's 4 x 4 block (tile row p // 4, tile column p % 4); empty slots hold -1. The positions of one device are distinct, its live slots come before its empty ones, a device has 4 to 12 live slots, and in every draw some device has all 12 live. Data in empty slots is not part of the image.
All inputs are finite; a program needn't handle non-finite values.
Results may differ from the reference program's by a relative error of at most 0.0003.
Values sent between devices are 32-bit elements; how exact they have to be, the bound alone decides.
No kernel may reach another device: no remote copies, remote signals or barrier semaphores. Data moves between devices by JAX's collectives and lax.ppermute only.
A program may use at most 128 MiB of HBM per device.

```python
import jax
import jax.numpy as jnp
from jax import lax

TILE = 256
BR = 4
BC = 4
SLOTS = 12
N_ROW = 8
N_COL = 16


def draw_slot_tile(key, part):
    devices = N_ROW * N_COL
    positions = BR * BC
    count_key = jax.random.fold_in(key, 11)
    order_key = jax.random.fold_in(key, 12)
    full_key = jax.random.fold_in(key, 13)
    counts = jax.random.randint(count_key, (devices,), SLOTS // 3, SLOTS + 1)
    busiest = jax.random.randint(full_key, (), 0, devices)
    counts = jnp.where(jnp.arange(devices) == busiest, SLOTS, counts)
    scores = jax.random.randint(order_key, (devices, positions), 0, 1 << 20) * positions + jnp.arange(positions)[None, :]
    ranked = jnp.argsort(scores, axis=1)[:, :SLOTS].astype(jnp.int32)
    filled = jnp.arange(SLOTS)[None, :] < counts[:, None]
    chosen = jnp.where(filled, ranked, -1)
    return chosen.reshape(N_ROW, N_COL * SLOTS).astype(jnp.int32)


def block_levels(stream_key, extent, split, low, high):
    gain = 1.0
    for dim, shards_of in split:
        heights = jax.random.uniform(jax.random.fold_in(jax.random.fold_in(stream_key, 6), dim), (shards_of,), jnp.float32, low / len(split), high / len(split))
        gain = gain * jnp.repeat(jnp.exp(heights), extent[dim] // shards_of).reshape((-1,) + (1,) * (len(extent) - 1 - dim))
    return gain


def setup_inputs(seed: int = 0) -> dict:
    key_of = jax.random.split(jax.random.key(seed), 3)
    return {
        "tiles": jnp.clip(0.02 + 0.98 * jax.random.uniform(key_of[0], (N_ROW, N_COL * SLOTS, 3, TILE, TILE), jnp.float32) ** block_levels(key_of[0], (N_ROW, N_COL * SLOTS, 3, TILE, TILE), ((0, 8), (1, 16)), -0.2, 0.2), 0.02, 1.0),
        "slot_tile": draw_slot_tile(jax.random.fold_in(key_of[2], 71), 0),
    }


PRECISE = lax.Precision.HIGHEST
WEIGHT_FLOOR = 0.25


def lanczos_matrix(shift, count_out, count_in):
    out_index = jnp.arange(count_out)[:, None]
    in_index = jnp.arange(count_in)[None, :]
    offset = (shift + in_index - 2 * out_index).astype(jnp.float32)
    scaled = (offset - 0.5) * 0.5
    kernel_raw = jnp.where(jnp.abs(scaled) < 3.0, jnp.sinc(scaled) * jnp.sinc(scaled / 3.0), 0.0)
    support = (jnp.arange(-5, 7).astype(jnp.float32) - 0.5) * 0.5
    weight_sum = jnp.sum(jnp.sinc(support) * jnp.sinc(support / 3.0))
    return (kernel_raw / weight_sum).astype(jnp.float32)


def resample(matrix_rows, matrix_cols, window):
    partial_value = jnp.einsum("jx,bxy->bjy", matrix_rows, window, precision=PRECISE)
    return jnp.einsum("bjy,ky->bjk", partial_value, matrix_cols, precision=PRECISE)


def finish(linear):
    weight = linear[3:4]
    colour = linear[:3] / jnp.maximum(weight, WEIGHT_FLOOR)
    opacity = jnp.clip(weight, 0.0, 1.0)
    display = jnp.concatenate([colour, opacity], axis=0)
    carried = jnp.concatenate([colour * opacity, opacity], axis=0)
    return display, carried


def first_level(tiles, slot_tile):
    half_side = TILE // 2
    rows_one = N_ROW * BR * half_side
    cols_one = N_COL * BC * half_side
    matrix = lanczos_matrix(6, half_side + 6, TILE)
    row_sums = jnp.sum(matrix, axis=1)
    opacity_patch = (row_sums[:, None] * row_sums[None, :])[None]
    flat_tiles = tiles.reshape(N_ROW * N_COL * SLOTS, 3, TILE, TILE)
    flat_slots = slot_tile.reshape(N_ROW * N_COL * SLOTS).astype(jnp.int32)
    anchor = jnp.zeros((), jnp.int32)

    def add_tile(index, canvas):
        index = jnp.asarray(index).astype(jnp.int32)
        position = flat_slots[index]
        filled = (position >= 0).astype(jnp.float32)
        place = jnp.maximum(position, 0)
        device = index // SLOTS
        tile_row = (device // N_COL) * BR + place // BC
        tile_col = (device % N_COL) * BC + place % BC
        data = lax.dynamic_index_in_dim(flat_tiles, index, 0, keepdims=False)
        patch = jnp.concatenate([resample(matrix, matrix, data), opacity_patch], axis=0) * filled
        start = (anchor, (tile_row * half_side).astype(jnp.int32), (tile_col * half_side).astype(jnp.int32))
        current = lax.dynamic_slice(canvas, start, patch.shape)
        return lax.dynamic_update_slice(canvas, current + patch, start)

    canvas = lax.fori_loop(0, N_ROW * N_COL * SLOTS, add_tile, jnp.zeros((4, rows_one + 6, cols_one + 6), jnp.float32))
    return canvas[:, 3:rows_one + 3, 3:cols_one + 3]


def reduce_level(state, block):
    channels, height, width = state.shape
    padded = jnp.pad(state, ((0, 0), (6, 6), (6, 6)))
    block_rows = height // 2 // block
    block_cols = width // 2 // block
    matrix = lanczos_matrix(-6, block, 2 * block + 12)
    anchor = jnp.zeros((), jnp.int32)

    def one_block(flat):
        band_row = flat // block_cols
        band_col = flat % block_cols
        start = (anchor, (band_row * 2 * block).astype(jnp.int32), (band_col * 2 * block).astype(jnp.int32))
        window = lax.dynamic_slice(padded, start, (channels, 2 * block + 12, 2 * block + 12))
        return resample(matrix, matrix, window)

    pieces = lax.map(one_block, jnp.arange(block_rows * block_cols).astype(jnp.int32))
    pieces = pieces.reshape(block_rows, block_cols, channels, block, block)
    return pieces.transpose(2, 0, 3, 1, 4).reshape(channels, height // 2, width // 2)


def reference(tiles, slot_tile):
    level_one, carried = finish(first_level(tiles, slot_tile))
    level_two, carried = finish(reduce_level(carried, TILE // 4))
    level_three, carried = finish(reduce_level(carried, TILE // 8))
    return level_one, level_two, level_three
```

```python
import jax
import jax.numpy as jnp
import numpy as np
from jax import lax
from jax.experimental import pallas as pl
from jax.experimental.pallas import tpu as pltpu
from jax.sharding import PartitionSpec as P

BR = 4
BC = 4
SLOTS = 12
TILE = 256
WEIGHT_FLOOR = 0.25

ROWS = 544
PATCH = 144
TOP = 24
PACK = 136
XPAD = 24
CPAD = 8
CROWS = 560
ROWS2 = 272


def lanczos(t):
    return np.where(np.abs(t) < 3.0, np.sinc(t) * np.sinc(t / 3.0), 0.0)


SUPPORT = lanczos((np.arange(-5, 7) - 0.5) / 2.0)
NORM = SUPPORT.sum()
TAPS = [float(np.float32(v / NORM)) for v in SUPPORT[5::-1]]


def taper(d):
    return (lanczos((d - 0.5) / 2.0) / NORM).astype(np.float32)


def split(matrix):
    high = matrix.astype(jnp.bfloat16)
    low = (matrix - high.astype(np.float32)).astype(jnp.bfloat16)
    return high, low


def tile_weights():
    x = np.arange(TILE)[:, None]
    lane = np.arange(128)[None, :]
    main = taper(x - 2 * lane)
    spill = np.where(lane < 8, taper(x - 2 * (lane + 128)), np.where(lane >= 120, taper(x - 2 * (lane - 128)), 0.0))
    spill = spill.astype(np.float32)
    mh, ml = split(main)
    sh, sl = split(spill)
    return np.stack([np.concatenate(pair, axis=1) for pair in ((mh, ml), (mh, sh), (sh, sl))])


def opacity_patch():
    x = np.arange(TILE)[None, :]
    rows = taper(x - 2 * np.arange(-8, PATCH - 8)[:, None]).sum(axis=1, dtype=np.float64)
    main = taper(x - 2 * np.arange(128)[:, None]).sum(axis=1, dtype=np.float64)
    lane = np.arange(128)
    right = taper(x - 2 * (lane[:, None] + 128)).sum(axis=1, dtype=np.float64)
    left = taper(x - 2 * (lane[:, None] - 128)).sum(axis=1, dtype=np.float64)
    cols = np.stack([main, np.where(lane >= 64, left, 0.0), np.where(lane < 64, right, 0.0)])
    return (cols[:, None, :] * rows[None, :, None]).astype(np.float32)


def wide_weights(own):
    edge = np.arange(128)
    cols_in = np.concatenate([np.arange(own), np.where(edge < 64, own + edge, edge - 128)])[:, None]
    cols_own = np.arange(own // 2)[None, :]
    cols_edge = np.where(edge < 64, own // 2 + edge, edge - 128)[None, :]
    return taper(cols_in - 2 * cols_own), taper(cols_in - 2 * cols_edge)


def level_two_weights():
    to_own, to_edge = wide_weights(512)
    oh, ol = split(to_own)
    eh, el = split(to_edge)
    zero = np.zeros((128, 128), eh.dtype)
    own = np.stack([oh[:512], ol[:512]])
    own_edge = np.concatenate([oh[512:], oh[512:], ol[512:], np.zeros((128, 256), oh.dtype)]).reshape(2, 256, 256)
    pick = lambda m: np.concatenate([m[:128], m[384:512]])
    edge = np.stack(
        [
            np.concatenate([pick(eh), pick(el)], axis=1),
            np.concatenate(
                [np.concatenate([eh[512:], el[512:]], axis=1), np.concatenate([eh[512:], zero], axis=1)]
            ),
        ]
    )
    return own, own_edge, edge


def level_three_weights():
    to_own, _ = wide_weights(256)
    oh, ol = split(to_own)
    zero = np.zeros((128, 128), oh.dtype)
    own = np.concatenate([oh[:256], ol[:256]], axis=1)
    edge = np.concatenate(
        [np.concatenate([oh[256:], ol[256:]], axis=1), np.concatenate([oh[256:], zero], axis=1)]
    )
    return np.stack([own, edge])


def fir(load, base, rows):
    total = None
    for k, weight in enumerate(TAPS):
        term = (load(base - k, rows) + load(base + 1 + k, rows)) * weight
        total = term if total is None else total + term
    return total


def halves(value):
    high = value.astype(jnp.bfloat16)
    return high, (value - high.astype(jnp.float32)).astype(jnp.bfloat16)


def dot(left, right):
    return jnp.dot(left, right, preferred_element_type=jnp.float32)


def tiles_kernel(slot_ref, tiles_ref, weight_ref, patch_ref, canvas_ref, up_ref, down_ref, x_ref, w_ref, p_ref, sem, wsem):
    def copies(s):
        return [
            pltpu.make_async_copy(
                tiles_ref.at[s, :, :, pl.ds(128 * b, 128)], x_ref.at[s, :, b, pl.ds(XPAD, TILE), :], sem.at[s, b]
            )
            for b in range(2)
        ]

    loads = [pltpu.make_async_copy(weight_ref, w_ref, wsem.at[0]), pltpu.make_async_copy(patch_ref, p_ref, wsem.at[1])]

    live = jnp.int32(0)
    for s in range(SLOTS):
        filled = slot_ref[0, s] >= 0
        live = live + filled.astype(jnp.int32)

        @pl.when(filled)
        def _():
            for copy in copies(s):
                copy.start()

        if s == 0:
            for copy in loads:
                copy.start()

    zero_pad = jnp.zeros((XPAD, 128), jnp.float32)

    def clear_pad(s, carry):
        for c in range(3):
            for b in range(2):
                x_ref[s, c, b, 0:XPAD, :] = zero_pad
                x_ref[s, c, b, XPAD + TILE : 2 * XPAD + TILE, :] = zero_pad
        return carry

    lax.fori_loop(0, SLOTS, clear_pad, 0)

    zero_rows = jnp.zeros((ROWS // 2, 128), jnp.float32)

    def clear(i, carry):
        c = i // 5
        b = i % 5
        canvas_ref[c, b, 0 : ROWS // 2, :] = zero_rows
        canvas_ref[c, b, ROWS // 2 : ROWS, :] = zero_rows
        return carry

    lax.fori_loop(0, 20, clear, 0)
    for copy in loads:
        copy.wait()

    lane = lax.broadcasted_iota(jnp.int32, (1, 128), 1)
    is_left = lane >= 64

    def add_tile(s, carry):
        place = slot_ref[0, s]
        tile_row = place // BC
        tile_col = place % BC
        left = jnp.where(tile_col == 0, 4, tile_col - 1)
        right = tile_col + 1
        rows = pl.ds(pl.multiple_of(tile_row * 128 + 8, 8), PATCH)
        for copy in copies(s):
            copy.wait()
        for c in range(3):
            highs, lows = [], []
            for chunk in range(PATCH // 16):
                base = 2 * (16 * chunk - 8) + XPAD
                pair = []
                for b in range(2):
                    load = lambda start, n, b=b: x_ref[s, c, b, pl.ds(start, n, stride=2), :]
                    pair.append(fir(load, base, 16))
                high, low = halves(jnp.concatenate(pair, axis=1))
                highs.append(high)
                lows.append(low)
            high = jnp.concatenate(highs, axis=0)
            low = jnp.concatenate(lows, axis=0)
            first = dot(high, w_ref[0])
            second = dot(low, w_ref[1])
            third = dot(high, w_ref[2])
            main = first[:, :128] + first[:, 128:] + second[:, :128]
            spill = second[:, 128:] + third[:, :128] + third[:, 128:]
            canvas_ref[c, tile_col, rows, :] += main
            canvas_ref[c, left, rows, :] += jnp.where(is_left, spill, 0.0)
            canvas_ref[c, right, rows, :] += jnp.where(is_left, 0.0, spill)
        canvas_ref[3, tile_col, rows, :] += p_ref[0]
        canvas_ref[3, left, rows, :] += p_ref[1]
        canvas_ref[3, right, rows, :] += p_ref[2]
        return carry

    lax.fori_loop(0, live, add_tile, 0)
    for c in range(4):
        for b in range(5):
            up_ref[c, b] = canvas_ref[c, b, 8:32, :]
            down_ref[c, b] = canvas_ref[c, b, 512:536, :]


def pack_kernel(canvas_ref, above_ref, below_ref, left_ref, right_ref):
    lane = lax.broadcasted_iota(jnp.int32, (1, 128), 1)
    is_left = lane >= 64

    def rows_of(c, b, start):
        if start == 0:
            head = canvas_ref[c, b, 0:TOP, :] + above_ref[c, b]
            return jnp.concatenate([head, canvas_ref[c, b, TOP:PACK, :]], axis=0)
        if start == 3 * PACK:
            tail = canvas_ref[c, b, ROWS - TOP : ROWS, :] + below_ref[c, b]
            return jnp.concatenate([canvas_ref[c, b, start : ROWS - TOP, :], tail], axis=0)
        return canvas_ref[c, b, start : start + PACK, :]

    for c in range(4):
        to_left = to_right = None
        for g in range(4):
            edge = rows_of(c, 4, g * PACK)
            band_left = jnp.where(is_left, edge, rows_of(c, 0, g * PACK))
            band_right = jnp.where(is_left, rows_of(c, 3, g * PACK), edge)
            band_left = pltpu.roll(band_left, 16 + 32 * g, 1)
            band_right = pltpu.roll(band_right, 16 + 32 * g, 1)
            if g == 0:
                to_left, to_right = band_left, band_right
            else:
                keep = lane < 32 * g
                to_left = jnp.where(keep, to_left, band_left)
                to_right = jnp.where(keep, to_right, band_right)
        left_ref[c] = to_left
        right_ref[c] = to_right


def levels_kernel(
    flag_ref, canvas_ref, above_ref, below_ref, from_left_ref, from_right_ref, own_ref, own_edge_ref, edge_ref, three_ref,
    one_out, two_out, three_out, add_ref, carried_ref, linear_ref, carried2_ref, one_ref, two_ref, three_stage, sem
):
    has_above = flag_ref[0]
    has_below = flag_ref[1]
    has_left = flag_ref[2]
    has_right = flag_ref[3]
    lane = lax.broadcasted_iota(jnp.int32, (1, 128), 1)
    is_left = lane >= 64
    edge_mask = jnp.where(is_left, has_left, has_right)

    zero_pad = jnp.zeros((CPAD, 128), jnp.float32)
    for c in range(4):
        for b in range(5):
            carried_ref[c, b, 0:CPAD, :] = zero_pad
            carried_ref[c, b, CPAD + ROWS : CROWS, :] = zero_pad

    in_band = (lane < 32 - 16) | (lane >= 128 - 16)
    for c in range(4):
        for g in range(4):
            shift = (128 - 16 - 32 * g) % 128
            add_ref[0, c, g * PACK : (g + 1) * PACK, :] = jnp.where(in_band, pltpu.roll(from_left_ref[c], shift, 1), 0.0)
            add_ref[1, c, g * PACK : (g + 1) * PACK, :] = jnp.where(in_band, pltpu.roll(from_right_ref[c], shift, 1), 0.0)

    def finish(linear):
        weight = linear[3]
        scale = 1.0 / jnp.maximum(weight, WEIGHT_FLOOR)
        opacity = jnp.clip(weight, 0.0, 1.0)
        colour = [linear[c] * scale for c in range(3)]
        return colour + [opacity], [value * opacity for value in colour] + [opacity]

    def finish_one(row, n, band, band_row, mask, out_row):
        rows = pl.ds(row, n)
        for b in range(5):
            linear = []
            for c in range(4):
                value = canvas_ref[c, b, rows, :]
                if band is not None:
                    value = value + band[c, b, pl.ds(band_row, n), :]
                if b == 0:
                    value = value + jnp.where(is_left, 0.0, add_ref[0, c, rows, :])
                if b == 3:
                    value = value + jnp.where(is_left, add_ref[1, c, rows, :], 0.0)
                if b == 4:
                    value = value + jnp.where(is_left, add_ref[0, c, rows, :], add_ref[1, c, rows, :])
                    value = value * edge_mask
                if mask is not None:
                    value = value * mask
                linear.append(value)
            shown, carried = finish(linear)
            for c in range(4):
                if b < 4 and out_row is not None:
                    one_ref[c, pl.ds(out_row, n), 128 * b : 128 * b + 128] = shown[c]
                carried_ref[c, b, pl.ds(row + CPAD, n), :] = carried[c]

    one_copies = [
        pltpu.make_async_copy(one_ref.at[:, pl.ds(128 * q, 128), :], one_out.at[:, pl.ds(128 * q, 128), :], sem.at[q])
        for q in range(4)
    ]
    finish_one(0, 16, above_ref, 0, has_above, None)
    finish_one(16, 8, above_ref, 16, None, 0)
    finish_one(24, 8, None, 0, None, 8)
    for q in range(4):
        def body(i, carry, q=q):
            out_row = pl.multiple_of(128 * q + 16 * i, 16)
            finish_one(out_row + 16, 16, None, 0, None, out_row)
            return carry

        lax.fori_loop(1 if q == 0 else 0, 7 if q == 3 else 8, body, 0)
        if q == 3:
            finish_one(512, 8, None, 0, None, 496)
            finish_one(520, 8, below_ref, 0, None, 504)
        one_copies[q].start()
    finish_one(528, 16, below_ref, 8, has_below, None)

    def reduce_two(c, carry):
        highs, lows = [], []
        for chunk in range(ROWS2 // 16):
            base = 2 * (16 * chunk - 8) + 16 + CPAD
            parts = [
                fir(lambda start, n, b=b: carried_ref[c, b, pl.ds(start, n, stride=2), :], base, 16) for b in range(5)
            ]
            high, low = halves(jnp.concatenate(parts, axis=1))
            highs.append(high)
            lows.append(low)
        high = jnp.concatenate(highs, axis=0)
        low = jnp.concatenate(lows, axis=0)
        both = jnp.concatenate([high[:, 512:], low[:, 512:]], axis=1)
        own = dot(high[:, :512], own_ref[0]) + dot(high[:, :512], own_ref[1]) + dot(low[:, :512], own_ref[0])
        own = own + dot(both, own_edge_ref[0]) + dot(high[:, 512:], own_edge_ref[1, :128, :])
        ends = jnp.concatenate([high[:, :128], high[:, 384:512]], axis=1)
        ends_low = jnp.concatenate([low[:, :128], low[:, 384:512]], axis=1)
        edge = dot(ends, edge_ref[0]) + dot(both, edge_ref[1])
        edge = edge[:, :128] + edge[:, 128:] + dot(ends_low, edge_ref[0, :, :128])
        linear_ref[c, 0] = own[:, :128]
        linear_ref[c, 1] = own[:, 128:]
        linear_ref[c, 2] = edge
        return carry

    lax.fori_loop(0, 4, reduce_two, 0)

    def finish_two(row, n, mask, out_row):
        rows = pl.ds(row, n)
        for b in range(3):
            linear = []
            for c in range(4):
                value = linear_ref[c, b, rows, :]
                if b == 2:
                    value = value * edge_mask
                if mask is not None:
                    value = value * mask
                linear.append(value)
            shown, carried = finish(linear)
            for c in range(4):
                if b < 2 and out_row is not None:
                    two_ref[c, pl.ds(out_row, n), 128 * b : 128 * b + 128] = shown[c]
                carried2_ref[c, b, rows, :] = carried[c]

    finish_two(0, 8, has_above, None)

    def body_two(i, carry):
        out_row = pl.multiple_of(16 * i, 16)
        finish_two(out_row + 8, 16, None, out_row)
        return carry

    lax.fori_loop(0, 16, body_two, 0)
    finish_two(264, 8, has_below, None)
    two_copy = pltpu.make_async_copy(two_ref, two_out, sem.at[4])
    two_copy.start()

    def reduce_three(c, carry):
        highs, lows = [], []
        for chunk in range(8):
            base = 2 * 16 * chunk + 8
            parts = [
                fir(lambda start, n, b=b: carried2_ref[c, b, pl.ds(start, n, stride=2), :], base, 16) for b in range(3)
            ]
            high, low = halves(jnp.concatenate(parts, axis=1))
            highs.append(high)
            lows.append(low)
        high = jnp.concatenate(highs, axis=0)
        low = jnp.concatenate(lows, axis=0)
        both = jnp.concatenate([high[:, 256:], low[:, 256:]], axis=1)
        total = dot(high[:, :256], three_ref[0]) + dot(both, three_ref[1])
        linear_ref[c, 0, 0:128, :] = total[:, :128] + total[:, 128:] + dot(low[:, :256], three_ref[0, :, :128])
        return carry

    lax.fori_loop(0, 4, reduce_three, 0)
    for row in range(0, 128, 16):
        shown, _ = finish([linear_ref[c, 0, row : row + 16, :] for c in range(4)])
        for c in range(4):
            three_stage[c, row : row + 16, :] = shown[c]
    three_copy = pltpu.make_async_copy(three_stage, three_out, sem.at[5])
    three_copy.start()
    for copy in one_copies:
        copy.wait()
    two_copy.wait()
    three_copy.wait()


VMEM = pl.BlockSpec(memory_space=pltpu.VMEM)
SMEM = pl.BlockSpec(memory_space=pltpu.SMEM)
HBM = pl.BlockSpec(memory_space=pltpu.HBM)
F32 = jnp.float32
BF16 = jnp.bfloat16


def params(mib):
    return pltpu.CompilerParams(vmem_limit_bytes=mib << 20)


def shifted(value, axis, steps):
    count = lax.axis_size(axis)
    pairs = [(i, i + steps) for i in range(count) if 0 <= i + steps < count]
    return lax.ppermute(value, axis, pairs)


def per_device(tiles, slot_tile):
    shape = jax.ShapeDtypeStruct
    canvas, up, down = pl.pallas_call(
        tiles_kernel,
        name="tiles",
        out_shape=(shape((4, 5, ROWS, 128), F32), shape((4, 5, TOP, 128), F32), shape((4, 5, TOP, 128), F32)),
        in_specs=[SMEM, HBM, HBM, HBM],
        out_specs=(VMEM, VMEM, VMEM),
        scratch_shapes=[
            pltpu.VMEM((SLOTS, 3, 2, TILE + 2 * XPAD, 128), F32),
            pltpu.VMEM((3, 256, 256), BF16),
            pltpu.VMEM((3, PATCH, 128), F32),
            pltpu.SemaphoreType.DMA((SLOTS, 2)),
            pltpu.SemaphoreType.DMA((2,)),
        ],
        compiler_params=params(30),
    )(slot_tile, tiles[0], jnp.asarray(tile_weights()), jnp.asarray(opacity_patch()))
    below = shifted(up, "row", -1)
    above = shifted(down, "row", 1)
    to_left, to_right = pl.pallas_call(
        pack_kernel,
        name="pack",
        out_shape=(shape((4, PACK, 128), F32), shape((4, PACK, 128), F32)),
        in_specs=[VMEM, VMEM, VMEM],
        out_specs=(VMEM, VMEM),
        compiler_params=params(20),
    )(canvas, above, below)
    from_right = shifted(to_left, "col", -1)
    from_left = shifted(to_right, "col", 1)
    row, col = lax.axis_index("row"), lax.axis_index("col")
    flags = jnp.stack([row > 0, row < lax.axis_size("row") - 1, col > 0, col < lax.axis_size("col") - 1]).astype(F32)
    own, own_edge, edge = level_two_weights()
    level_one, level_two, level_three = pl.pallas_call(
        levels_kernel,
        name="levels",
        out_shape=(shape((4, 512, 512), F32), shape((4, 256, 256), F32), shape((4, 128, 128), F32)),
        in_specs=[SMEM] + [VMEM] * 9,
        out_specs=(HBM, HBM, HBM),
        scratch_shapes=[
            pltpu.VMEM((2, 4, ROWS, 128), F32),
            pltpu.VMEM((4, 5, CROWS, 128), F32),
            pltpu.VMEM((4, 3, ROWS2, 128), F32),
            pltpu.VMEM((4, 3, ROWS2, 128), F32),
            pltpu.VMEM((4, 512, 512), F32),
            pltpu.VMEM((4, 256, 256), F32),
            pltpu.VMEM((4, 128, 128), F32),
            pltpu.SemaphoreType.DMA((6,)),
        ],
        compiler_params=params(30),
    )(
        flags, canvas, above, below, from_left, from_right,
        jnp.asarray(own), jnp.asarray(own_edge), jnp.asarray(edge), jnp.asarray(level_three_weights()),
    )
    return (level_one, level_two, level_three)


def solution(mesh):
    placed = (P("row", "col", None, None, None), P("row", "col"))
    return jax.shard_map(
        per_device,
        mesh=mesh,
        in_specs=placed,
        out_specs=(P(None, "row", "col"), P(None, "row", "col"), P(None, "row", "col")),
        check_vma=False,
    )
```

```python
import jax
import jax.numpy as jnp
import numpy as np
from jax import lax
from jax.experimental import pallas as pl
from jax.experimental.pallas import tpu as pltpu
from jax.sharding import PartitionSpec as P

BR = 4
BC = 4
SLOTS = 12
TILE = 256
WEIGHT_FLOOR = 0.25

ROWS = 544
HALF = 160
INNER = 288
PATCH = 144
TOP = 24
BAND = 18
GROUPS = 7
PACK = 80
XPAD = 24
CPAD = 8
CROWS = 560
ROWS2 = 272


def lanczos(t):
    return np.where(np.abs(t) < 3.0, np.sinc(t) * np.sinc(t / 3.0), 0.0)


SUPPORT = lanczos((np.arange(-5, 7) - 0.5) / 2.0)
NORM = SUPPORT.sum()
TAPS = [float(np.float32(v / NORM)) for v in SUPPORT[5::-1]]


def taper(d):
    return (lanczos((d - 0.5) / 2.0) / NORM).astype(np.float32)


def split(matrix):
    high = matrix.astype(jnp.bfloat16)
    low = (matrix - high.astype(np.float32)).astype(jnp.bfloat16)
    return high, low


def tile_weights():
    x = np.arange(TILE)[:, None]
    lane = np.arange(128)[None, :]
    main = taper(x - 2 * lane)
    spill = np.where(lane < 8, taper(x - 2 * (lane + 128)), np.where(lane >= 120, taper(x - 2 * (lane - 128)), 0.0))
    spill = spill.astype(np.float32)
    mh, ml = split(main)
    sh, sl = split(spill)
    return np.stack([np.concatenate(pair, axis=1) for pair in ((mh, ml), (mh, sh), (sh, sl))])


def opacity_patch():
    x = np.arange(TILE)[None, :]
    rows = taper(x - 2 * np.arange(-8, PATCH - 8)[:, None]).sum(axis=1, dtype=np.float64)
    main = taper(x - 2 * np.arange(128)[:, None]).sum(axis=1, dtype=np.float64)
    lane = np.arange(128)
    right = taper(x - 2 * (lane[:, None] + 128)).sum(axis=1, dtype=np.float64)
    left = taper(x - 2 * (lane[:, None] - 128)).sum(axis=1, dtype=np.float64)
    cols = np.stack([main, np.where(lane >= 64, left, 0.0), np.where(lane < 64, right, 0.0)])
    return (cols[:, None, :] * rows[None, :, None]).astype(np.float32)


def wide_weights(own):
    edge = np.arange(128)
    cols_in = np.concatenate([np.arange(own), np.where(edge < 64, own + edge, edge - 128)])[:, None]
    cols_own = np.arange(own // 2)[None, :]
    cols_edge = np.where(edge < 64, own // 2 + edge, edge - 128)[None, :]
    return taper(cols_in - 2 * cols_own), taper(cols_in - 2 * cols_edge)


def level_two_weights():
    oh, ol = split(wide_weights(512)[0])
    eh, el = split(wide_weights(512)[1])
    th, tl = split(wide_weights(256)[0])
    zero = np.zeros((128, 128), eh.dtype)
    ends = lambda m: np.concatenate([m[:128], m[384:512]])
    beside = lambda *parts: np.concatenate(parts, axis=1)
    rest = [
        ends(oh),
        ends(ol),
        np.concatenate([oh[512:], oh[512:]]),
        np.concatenate([ol[512:], ol[512:]]),
        beside(ends(eh), ends(el)),
        np.concatenate([beside(eh[512:], el[512:]), beside(eh[512:], zero)]),
        beside(th[:256], tl[:256]),
        np.concatenate([beside(th[256:], tl[256:]), beside(th[256:], zero)]),
    ]
    return np.stack([oh[128:384], ol[128:384]]), np.stack(rest)


def fir(load, count, row0):
    rows = {}

    def at(t):
        if t not in rows:
            rows[t] = load(t)
        return rows[t]

    results = []
    for q in range(count):
        total = None
        for k, weight in enumerate(TAPS):
            term = (at(row0 + 2 * q - k) + at(row0 + 2 * q + 1 + k)) * weight
            total = term if total is None else total + term
        results.append(total)
    return results


def halves(value):
    high = value.astype(jnp.bfloat16)
    return high, (value - high.astype(jnp.float32)).astype(jnp.bfloat16)


def split_columns(parts):
    count = len(parts[0])
    highs, lows = [], []
    for q in range(0, count, 2):
        rows = [jnp.concatenate([part[p] for part in parts], axis=1) for p in range(q, min(q + 2, count))]
        high, low = halves(jnp.concatenate(rows, axis=0))
        highs.append(high)
        lows.append(low)
    return jnp.concatenate(highs, axis=0), jnp.concatenate(lows, axis=0)


def dot(left, right):
    return jnp.dot(left, right, preferred_element_type=jnp.float32)


def add_tiles(slot_ref, tiles_ref, weight_ref, patch_ref, canvas_ref, x_ref, v_ref, w_ref, p_ref, list_ref, sem, wsem, outer, before):
    def copies(s, i):
        return [
            pltpu.make_async_copy(
                tiles_ref.at[s, :, :, pl.ds(128 * b, 128)], x_ref.at[i, :, b, pl.ds(XPAD, TILE), :], sem.at[i, b]
            )
            for b in range(2)
        ]

    loads = [pltpu.make_async_copy(weight_ref, w_ref, wsem.at[0]), pltpu.make_async_copy(patch_ref, p_ref, wsem.at[1])]
    count = jnp.int32(0)
    for s in range(SLOTS):
        place = slot_ref[0, s]
        tile_row = place >> 2
        if outer:
            wanted = (place >= 0) & ((tile_row == 0) | (tile_row == BR - 1))
        else:
            wanted = (tile_row == 1) | (tile_row == 2)

        @pl.when(wanted)
        def _(s=s, count=count):
            list_ref[count] = s
            for copy in copies(s, count):
                copy.start()

        count = count + wanted.astype(jnp.int32)
        if s == 0:
            for copy in loads:
                copy.start()

    zero_pad = jnp.zeros((XPAD, 128), jnp.float32)

    def clear_pad(i, carry):
        for c in range(3):
            for b in range(2):
                x_ref[i, c, b, 0:XPAD, :] = zero_pad
                x_ref[i, c, b, XPAD + TILE : 2 * XPAD + TILE, :] = zero_pad
        return carry

    lax.fori_loop(0, count, clear_pad, 0)
    before()
    for copy in loads:
        copy.wait()

    lane = lax.broadcasted_iota(jnp.int32, (1, 128), 1)
    is_left = lane >= 64
    steps = PATCH // 8

    def arrive(i):
        for copy in copies(list_ref[i], i):
            copy.wait()

    def vertical(i):
        for c in range(3):
            parts = [
                fir(lambda t, b=b: x_ref[i, c, b, pl.ds(t, 8, stride=2 * steps), :], steps, XPAD - 16) for b in range(2)
            ]
            v_ref[0, c], v_ref[1, c] = split_columns(parts)

    def horizontal(i):
        place = slot_ref[0, list_ref[i]]
        tile_row = place >> 2
        tile_col = place & 3
        blocks = (tile_col, jnp.where(tile_col == 0, 4, tile_col - 1), tile_col + 1)
        row0 = pl.multiple_of(jnp.where(tile_row == 0, 8, HALF + 8) if outer else tile_row * 128 - 120, 8)

        def add(c, rows, values):
            olds = [[canvas_ref[c, block, r, :] for r in rows] for block in blocks]
            for block, old, new in zip(blocks, olds, values):
                for r, first, second in zip(rows, old, new):
                    canvas_ref[c, block, r, :] = first + second

        for r in range(0, PATCH, 48):
            values = [[p_ref[k, r + t : r + t + 8, :] for t in range(0, 48, 8)] for k in range(3)]
            add(3, [pl.ds(row0 + r + t, 8) for t in range(0, 48, 8)], values)
        for c in range(3):
            first = dot(v_ref[0, c], w_ref[0])
            second = dot(v_ref[1, c], w_ref[1])
            third = dot(v_ref[0, c], w_ref[2])
            main = first[:, :128] + first[:, 128:] + second[:, :128]
            spill = second[:, 128:] + third[:, :128] + third[:, 128:]
            for q0 in range(0, steps, 6):
                mains = [main[8 * q : 8 * q + 8] for q in range(q0, q0 + 6)]
                spills = [spill[8 * q : 8 * q + 8] for q in range(q0, q0 + 6)]
                values = (mains, [jnp.where(is_left, v, 0.0) for v in spills], [jnp.where(is_left, 0.0, v) for v in spills])
                add(c, [pl.ds(row0 + q, 8, stride=steps) for q in range(q0, q0 + 6)], values)

    @pl.when(count > 0)
    def _():
        arrive(0)
        vertical(0)

        def step(i, carry):
            arrive(i)
            horizontal(i - 1)
            vertical(i)
            return carry

        lax.fori_loop(1, count, step, 0)
        horizontal(count - 1)


def clear_canvas(canvas_ref, count):
    zero_rows = jnp.zeros((count // 2, 128), jnp.float32)

    def clear(i, carry):
        c = i // 5
        b = i % 5
        canvas_ref[c, b, 0 : count // 2, :] = zero_rows
        canvas_ref[c, b, count // 2 : count, :] = zero_rows
        return carry

    lax.fori_loop(0, 20, clear, 0)


def outer_kernel(slot_ref, tiles_ref, weight_ref, patch_ref, canvas_ref, up_ref, down_ref, *scratch):
    clear = lambda: clear_canvas(canvas_ref, 2 * HALF)
    add_tiles(slot_ref, tiles_ref, weight_ref, patch_ref, canvas_ref, *scratch, True, clear)
    for c in range(4):
        for b in range(5):
            up_ref[c, b] = canvas_ref[c, b, 8:32, :]
            down_ref[c, b] = canvas_ref[c, b, HALF + 128 : HALF + 152, :]


def inner_kernel(slot_ref, tiles_ref, weight_ref, patch_ref, canvas_ref, *scratch):
    clear = lambda: clear_canvas(canvas_ref, INNER)
    add_tiles(slot_ref, tiles_ref, weight_ref, patch_ref, canvas_ref, *scratch, False, clear)


def canvas_rows(outer_ref, inner_ref, c, b, row, n, kind):
    value = None
    if kind != 2:
        value = outer_ref[c, b, pl.ds(row if kind < 2 else row - (384 - HALF), n), :]
    if kind in (1, 2, 3):
        more = inner_ref[c, b, pl.ds(row - 128, n), :]
        value = more if value is None else value + more
    return value


KINDS = ((0, 128, 0), (128, 160, 1), (160, 384, 2), (384, 416, 3), (416, 544, 4))


def pack_kernel(outer_ref, inner_ref, above_ref, below_ref, left_ref, right_ref):
    lane = lax.broadcasted_iota(jnp.int32, (1, 128), 1)
    is_left = lane >= 64

    def rows_of(c, b, start):
        stop = min(start + PACK, ROWS)
        pieces = []
        for low, high, kind in KINDS:
            first, last = max(low, start), min(high, stop)
            if first < last:
                pieces.append(canvas_rows(outer_ref, inner_ref, c, b, first, last - first, kind))
        value = jnp.concatenate(pieces, axis=0) if len(pieces) > 1 else pieces[0]
        if start == 0:
            value = jnp.concatenate([value[:TOP] + above_ref[c, b], value[TOP:]], axis=0)
        if stop == ROWS:
            value = jnp.concatenate([value[:-TOP], value[-TOP:] + below_ref[c, b]], axis=0)
        return value

    for c in range(4):
        for out_ref, block, first in ((left_ref, 0, 3), (right_ref, 3, 15)):
            packed = None
            for g in range(GROUPS):
                edge, own = rows_of(c, 4, g * PACK), rows_of(c, block, g * PACK)
                band = jnp.where(is_left, edge, own) if block == 0 else jnp.where(is_left, own, edge)
                band = pltpu.roll(band, (first + BAND * g) % 128, 1)
                if packed is None:
                    packed = band
                elif band.shape == packed.shape:
                    packed = jnp.where(lane < BAND * g, packed, band)
                else:
                    rows = band.shape[0]
                    band = jnp.where(lane < BAND * g, packed[:rows], band)
                    packed = jnp.concatenate([band, packed[rows:]], axis=0)
            out_ref[c] = packed


def finish(linear):
    weight = linear[3]
    scale = 1.0 / jnp.maximum(weight, WEIGHT_FLOOR)
    opacity = jnp.clip(weight, 0.0, 1.0)
    colour = [linear[c] * scale for c in range(3)]
    return colour + [opacity], [value * opacity for value in colour] + [opacity]


def level_one_rows(flag_ref, above_ref, below_ref, finish_one, copies):
    has_above, has_below = flag_ref[0], flag_ref[1]

    def run(low, high, kind):
        def body(i, carry):
            row = pl.multiple_of(low + 16 * i, 16)
            finish_one(row, 16, None, 0, None, row - 16, kind)
            return carry

        lax.fori_loop(0, (high - low) // 16, body, 0)

    finish_one(0, 16, above_ref, 0, has_above, None, 0)
    finish_one(16, 8, above_ref, 16, None, 0, 0)
    finish_one(24, 8, None, 0, None, 8, 0)
    run(32, 128, 0)
    run(128, 160, 1)
    run(160, 272, 2)
    for copy in copies[0]:
        copy.start()
    run(272, 384, 2)
    run(384, 416, 3)
    run(416, 512, 4)
    finish_one(512, 8, None, 0, None, 496, 4)
    finish_one(520, 8, below_ref, 0, None, 504, 4)
    for copy in copies[1]:
        copy.start()
    finish_one(528, 16, below_ref, 8, has_below, None, 4)


def clear_carried(carried_ref, blocks):
    zero_pad = jnp.zeros((CPAD, 128), jnp.float32)
    for c in range(4):
        for b in range(blocks):
            carried_ref[c, b, 0:CPAD, :] = zero_pad
            carried_ref[c, b, CPAD + ROWS : CROWS, :] = zero_pad


STEPS2 = ROWS2 // 8
STEPS3 = 17


def middle_kernel(flag_ref, outer_ref, inner_ref, above_ref, below_ref, own_hbm, one_out, part_ref, carried_ref, one_ref, own_ref, sem):
    load = pltpu.make_async_copy(own_hbm, own_ref, sem.at[2])
    load.start()
    clear_carried(carried_ref, 2)

    def finish_one(row, n, band, band_row, mask, out_row, kind):
        for b in range(2):
            linear = []
            for c in range(4):
                value = canvas_rows(outer_ref, inner_ref, c, b + 1, row, n, kind)
                if band is not None:
                    value = value + band[c, b + 1, pl.ds(band_row, n), :]
                if mask is not None:
                    value = value * mask
                linear.append(value)
            shown, carried = finish(linear)
            for c in range(4):
                if out_row is not None:
                    one_ref[c, pl.ds(out_row, n), 128 * b : 128 * b + 128] = shown[c]
                carried_ref[c, b, pl.ds(row + CPAD, n), :] = carried[c]

    copies = [
        [
            pltpu.make_async_copy(
                one_ref.at[:, pl.ds(256 * q, 256), :], one_out.at[:, pl.ds(256 * q, 256), pl.ds(128, 256)], sem.at[q]
            )
        ]
        for q in range(2)
    ]
    level_one_rows(flag_ref, above_ref, below_ref, finish_one, copies)
    load.wait()

    def reduce_two(c, carry):
        parts = [
            fir(lambda t, b=b: carried_ref[c, b, pl.ds(t, 8, stride=2 * STEPS2), :], STEPS2, CPAD) for b in range(2)
        ]
        high, low = split_columns(parts)
        own = dot(high, own_ref[0]) + dot(high, own_ref[1]) + dot(low, own_ref[0])
        part_ref[c, 0] = own[:, :128]
        part_ref[c, 1] = own[:, 128:]
        return carry

    lax.fori_loop(0, 4, reduce_two, 0)
    for pair in copies:
        for copy in pair:
            copy.wait()


def levels_kernel(
    flag_ref, outer_ref, inner_ref, above_ref, below_ref, from_left_ref, from_right_ref, part_ref, own_hbm, one_in,
    one_out, two_out, three_out,
    add_ref, carried_ref, linear_ref, carried2_ref, one_ref, two_ref, three_stage, w_ref, sem,
):
    load = pltpu.make_async_copy(own_hbm, w_ref, sem.at[6])
    load.start()
    has_above, has_below, has_left, has_right = flag_ref[0], flag_ref[1], flag_ref[2], flag_ref[3]
    lane = lax.broadcasted_iota(jnp.int32, (1, 128), 1)
    is_left = lane >= 64
    edge_mask = jnp.where(is_left, has_left, has_right)
    clear_carried(carried_ref, 3)
    for c in range(4):
        for b in range(3):
            carried2_ref[c, b, ROWS2 : ROWS2 + 16, :] = jnp.zeros((16, 128), jnp.float32)

    from_left_lanes = (lane >= 113) | (lane < 3)
    from_right_lanes = (lane >= 125) | (lane < 15)
    for c in range(4):
        for side, ref, first, lanes in ((0, from_left_ref, 15, from_left_lanes), (1, from_right_ref, 3, from_right_lanes)):
            for g in range(GROUPS):
                start, stop = g * PACK, min(g * PACK + PACK, ROWS)
                band = pltpu.roll(ref[c, 0 : stop - start, :], (-first - BAND * g) % 128, 1)
                add_ref[side, c, start:stop, :] = jnp.where(lanes, band, 0.0)

    def finish_one(row, n, band, band_row, mask, out_row, kind):
        rows = pl.ds(row, n)
        for b, block in enumerate((0, 3, 4)):
            linear = []
            for c in range(4):
                value = canvas_rows(outer_ref, inner_ref, c, block, row, n, kind)
                if band is not None:
                    value = value + band[c, block, pl.ds(band_row, n), :]
                if b == 0:
                    value = value + jnp.where(is_left, 0.0, add_ref[0, c, rows, :])
                if b == 1:
                    value = value + jnp.where(is_left, add_ref[1, c, rows, :], 0.0)
                if b == 2:
                    value = value + jnp.where(is_left, add_ref[0, c, rows, :], add_ref[1, c, rows, :])
                    value = value * edge_mask
                if mask is not None:
                    value = value * mask
                linear.append(value)
            shown, carried = finish(linear)
            for c in range(4):
                if b < 2 and out_row is not None:
                    one_ref[b, c, pl.ds(out_row, n), :] = shown[c]
                carried_ref[c, b, pl.ds(row + CPAD, n), :] = carried[c]

    copies = [
        [
            pltpu.make_async_copy(
                one_ref.at[b, :, pl.ds(256 * q, 256), :],
                one_out.at[:, pl.ds(256 * q, 256), pl.ds(384 * b, 128)],
                sem.at[2 * q + b],
            )
            for b in range(2)
        ]
        for q in range(2)
    ]
    level_one_rows(flag_ref, above_ref, below_ref, finish_one, copies)
    load.wait()

    def reduce_two(c, carry):
        parts = [
            fir(lambda t, b=b: carried_ref[c, b, pl.ds(t, 8, stride=2 * STEPS2), :], STEPS2, CPAD) for b in range(3)
        ]
        high, low = split_columns(parts)
        ends, ends_low = high[:, :256], low[:, :256]
        both = jnp.concatenate([high[:, 256:], low[:, 256:]], axis=1)
        own = dot(ends, w_ref[0]) + dot(ends, w_ref[1]) + dot(ends_low, w_ref[0])
        own = own + dot(both, w_ref[2]) + dot(high[:, 256:], w_ref[3, :128, :])
        edge = dot(ends, w_ref[4]) + dot(both, w_ref[5])
        edge = edge[:, :128] + edge[:, 128:] + dot(ends_low, w_ref[4, :, :128])
        own_left = own[:, :128] + part_ref[c, 0]
        own_right = own[:, 128:] + part_ref[c, 1]
        for q in range(STEPS2):
            rows = pl.ds(q, 8, stride=STEPS2)
            linear_ref[c, 0, rows, :] = own_left[8 * q : 8 * q + 8]
            linear_ref[c, 1, rows, :] = own_right[8 * q : 8 * q + 8]
            linear_ref[c, 2, rows, :] = edge[8 * q : 8 * q + 8]
        return carry

    lax.fori_loop(0, 4, reduce_two, 0)

    def finish_two(row, n, mask, out_row):
        rows = pl.ds(row, n)
        for b in range(3):
            linear = []
            for c in range(4):
                value = linear_ref[c, b, rows, :]
                if b == 2:
                    value = value * edge_mask
                if mask is not None:
                    value = value * mask
                linear.append(value)
            shown, carried = finish(linear)
            for c in range(4):
                if b < 2 and out_row is not None:
                    two_ref[c, pl.ds(out_row, n), 128 * b : 128 * b + 128] = shown[c]
                carried2_ref[c, b, rows, :] = carried[c]

    finish_two(0, 8, has_above, None)

    def body_two(i, carry):
        out_row = pl.multiple_of(16 * i, 16)
        finish_two(out_row + 8, 16, None, out_row)
        return carry

    lax.fori_loop(0, 16, body_two, 0)
    finish_two(264, 8, has_below, None)
    two_copy = pltpu.make_async_copy(two_ref, two_out, sem.at[4])
    two_copy.start()

    def reduce_three(c, carry):
        parts = [
            fir(lambda t, b=b: carried2_ref[c, b, pl.ds(t, 8, stride=2 * STEPS3), :], STEPS3, 8) for b in range(3)
        ]
        high, low = split_columns(parts)
        both = jnp.concatenate([high[:, 256:], low[:, 256:]], axis=1)
        total = dot(high[:, :256], w_ref[6]) + dot(both, w_ref[7])
        total = total[:, :128] + total[:, 128:] + dot(low[:, :256], w_ref[6, :, :128])
        for q in range(STEPS3):
            linear_ref[c, 0, pl.ds(q, 8, stride=STEPS3), :] = total[8 * q : 8 * q + 8]
        return carry

    lax.fori_loop(0, 4, reduce_three, 0)
    for row in range(0, 128, 16):
        shown, _ = finish([linear_ref[c, 0, row : row + 16, :] for c in range(4)])
        for c in range(4):
            three_stage[c, row : row + 16, :] = shown[c]
    three_copy = pltpu.make_async_copy(three_stage, three_out, sem.at[5])
    three_copy.start()
    for pair in copies:
        for copy in pair:
            copy.wait()
    two_copy.wait()
    three_copy.wait()


VMEM = pl.BlockSpec(memory_space=pltpu.VMEM)
SMEM = pl.BlockSpec(memory_space=pltpu.SMEM)
HBM = pl.BlockSpec(memory_space=pltpu.HBM)
F32 = jnp.float32
BF16 = jnp.bfloat16


def params(mib):
    return pltpu.CompilerParams(vmem_limit_bytes=mib << 20)


def shifted(value, axis, steps):
    count = lax.axis_size(axis)
    pairs = [(i, i + steps) for i in range(count) if 0 <= i + steps < count]
    return lax.ppermute(value, axis, pairs)


def per_device(tiles, slot_tile):
    shape = jax.ShapeDtypeStruct
    band_shape = pltpu.VMEM((4, 5, TOP, 128), F32)
    pack_shape = pltpu.VMEM((4, PACK, 128), F32)
    in_hbm = lambda value: pltpu.with_memory_space_constraint(value, pltpu.HBM)
    weights, patch = in_hbm(jnp.asarray(tile_weights())), in_hbm(jnp.asarray(opacity_patch()))
    data = in_hbm(tiles[0])
    scratch = [
        pltpu.VMEM((8, 3, 2, TILE + 2 * XPAD, 128), F32),
        pltpu.VMEM((2, 3, PATCH, 256), BF16),
        pltpu.VMEM((3, 256, 256), BF16),
        pltpu.VMEM((3, PATCH, 128), F32),
        pltpu.SMEM((SLOTS,), jnp.int32),
        pltpu.SemaphoreType.DMA((8, 2)),
        pltpu.SemaphoreType.DMA((2,)),
    ]
    outer, up, down = pl.pallas_call(
        outer_kernel,
        name="outer",
        out_shape=(pltpu.VMEM((4, 5, 2 * HALF, 128), F32), band_shape, band_shape),
        in_specs=[SMEM, HBM, HBM, HBM],
        out_specs=(VMEM, VMEM, VMEM),
        scratch_shapes=scratch,
        compiler_params=params(30),
    )(slot_tile, data, weights, patch)
    below = shifted(up, "row", -1)
    above = shifted(down, "row", 1)
    inner = pl.pallas_call(
        inner_kernel,
        name="inner",
        out_shape=pltpu.VMEM((4, 5, INNER, 128), F32),
        in_specs=[SMEM, HBM, HBM, HBM],
        out_specs=VMEM,
        scratch_shapes=scratch,
        cost_estimate=pl.CostEstimate(flops=4_000_000_000, bytes_accessed=4_000_000, transcendentals=0),
        compiler_params=params(30),
    )(slot_tile, data, weights, patch)
    to_left, to_right = pl.pallas_call(
        pack_kernel,
        name="pack",
        out_shape=(pack_shape, pack_shape),
        in_specs=[VMEM] * 4,
        out_specs=(VMEM, VMEM),
        compiler_params=params(20),
    )(outer, inner, above, below)
    from_right = shifted(to_left, "col", -1)
    from_left = shifted(to_right, "col", 1)
    row, col = lax.axis_index("row"), lax.axis_index("col")
    flags = jnp.stack([row > 0, row < lax.axis_size("row") - 1, col > 0, col < lax.axis_size("col") - 1]).astype(F32)
    middle, rest = level_two_weights()
    level_one, part = pl.pallas_call(
        middle_kernel,
        name="middle",
        out_shape=(shape((4, 512, 512), F32), pltpu.VMEM((4, 2, ROWS2, 128), F32)),
        in_specs=[SMEM, VMEM, VMEM, VMEM, VMEM, HBM],
        out_specs=(HBM, VMEM),
        scratch_shapes=[
            pltpu.VMEM((4, 2, CROWS, 128), F32),
            pltpu.VMEM((4, 512, 256), F32),
            pltpu.VMEM((2, 256, 256), BF16),
            pltpu.SemaphoreType.DMA((3,)),
        ],
        cost_estimate=pl.CostEstimate(flops=4_000_000_000, bytes_accessed=4_000_000, transcendentals=0),
        compiler_params=params(30),
    )(flags, outer, inner, above, below, in_hbm(jnp.asarray(middle)))
    return pl.pallas_call(
        levels_kernel,
        name="levels",
        out_shape=(shape((4, 512, 512), F32), shape((4, 256, 256), F32), shape((4, 128, 128), F32)),
        in_specs=[SMEM] + [VMEM] * 7 + [HBM, HBM],
        out_specs=(HBM, HBM, HBM),
        scratch_shapes=[
            pltpu.VMEM((2, 4, ROWS, 128), F32),
            pltpu.VMEM((4, 3, CROWS, 128), F32),
            pltpu.VMEM((4, 3, ROWS2, 128), F32),
            pltpu.VMEM((4, 3, ROWS2 + 16, 128), F32),
            pltpu.VMEM((2, 4, 512, 128), F32),
            pltpu.VMEM((4, 256, 256), F32),
            pltpu.VMEM((4, 128, 128), F32),
            pltpu.VMEM((8, 256, 256), BF16),
            pltpu.SemaphoreType.DMA((7,)),
        ],
        input_output_aliases={9: 0},
        compiler_params=params(30),
    )(flags, outer, inner, above, below, from_left, from_right, part, in_hbm(jnp.asarray(rest)), level_one)


def solution(mesh):
    placed = (P("row", "col", None, None, None), P("row", "col"))
    return jax.shard_map(
        per_device,
        mesh=mesh,
        in_specs=placed,
        out_specs=(P(None, "row", "col"), P(None, "row", "col"), P(None, "row", "col")),
        check_vma=False,
    )
```

```python
import jax
import jax.numpy as jnp
import numpy as np
from jax import lax
from jax.experimental import pallas as pl
from jax.experimental.pallas import tpu as pltpu
from jax.sharding import PartitionSpec as P

BR = 4
BC = 4
SLOTS = 12
TILE = 256
WEIGHT_FLOOR = 0.25

ROWS = 544
INNER = 288
QUOTA = 8
PATCH = 144
TOP = 24
BAND = 18
GROUPS = 7
PACK = 80
XPAD = 24
CPAD = 8
CROWS = 560
ROWS2 = 272


def lanczos(t):
    return np.where(np.abs(t) < 3.0, np.sinc(t) * np.sinc(t / 3.0), 0.0)


SUPPORT = lanczos((np.arange(-5, 7) - 0.5) / 2.0)
NORM = SUPPORT.sum()
TAPS = [float(np.float32(v / NORM)) for v in SUPPORT[5::-1]]


def taper(d):
    return (lanczos((d - 0.5) / 2.0) / NORM).astype(np.float32)


def split(matrix):
    high = matrix.astype(jnp.bfloat16)
    low = (matrix - high.astype(np.float32)).astype(jnp.bfloat16)
    return high, low


def tile_weights():
    x = np.arange(TILE)[:, None]
    lane = np.arange(128)[None, :]
    main = taper(x - 2 * lane)
    spill = np.where(lane < 8, taper(x - 2 * (lane + 128)), np.where(lane >= 120, taper(x - 2 * (lane - 128)), 0.0))
    spill = spill.astype(np.float32)
    mh, ml = split(main)
    sh, sl = split(spill)
    return np.stack([np.concatenate(pair, axis=1) for pair in ((mh, ml), (mh, sh), (sh, sl))])


def opacity_patch():
    x = np.arange(TILE)[None, :]
    rows = taper(x - 2 * np.arange(-8, PATCH - 8)[:, None]).sum(axis=1, dtype=np.float64)
    main = taper(x - 2 * np.arange(128)[:, None]).sum(axis=1, dtype=np.float64)
    lane = np.arange(128)
    right = taper(x - 2 * (lane[:, None] + 128)).sum(axis=1, dtype=np.float64)
    left = taper(x - 2 * (lane[:, None] - 128)).sum(axis=1, dtype=np.float64)
    cols = np.stack([main, np.where(lane >= 64, left, 0.0), np.where(lane < 64, right, 0.0)])
    return (cols[:, None, :] * rows[None, :, None]).astype(np.float32)


def wide_weights(own):
    edge = np.arange(128)
    cols_in = np.concatenate([np.arange(own), np.where(edge < 64, own + edge, edge - 128)])[:, None]
    cols_own = np.arange(own // 2)[None, :]
    cols_edge = np.where(edge < 64, own // 2 + edge, edge - 128)[None, :]
    return taper(cols_in - 2 * cols_own), taper(cols_in - 2 * cols_edge)


def level_two_weights():
    oh, ol = split(wide_weights(512)[0])
    eh, el = split(wide_weights(512)[1])
    th, tl = split(wide_weights(256)[0])
    zero = np.zeros((128, 128), eh.dtype)
    ends = lambda m: np.concatenate([m[:128], m[384:512]])
    beside = lambda *parts: np.concatenate(parts, axis=1)
    rest = [
        ends(oh),
        ends(ol),
        np.concatenate([oh[512:], oh[512:]]),
        np.concatenate([ol[512:], ol[512:]]),
        beside(ends(eh), ends(el)),
        np.concatenate([beside(eh[512:], el[512:]), beside(eh[512:], zero)]),
        beside(th[:256], tl[:256]),
        np.concatenate([beside(th[256:], tl[256:]), beside(th[256:], zero)]),
    ]
    return np.stack([oh[128:384], ol[128:384]]), np.stack(rest)


def fir(load, count, row0):
    rows = {}

    def at(t):
        if t not in rows:
            rows[t] = load(t)
        return rows[t]

    results = []
    for q in range(count):
        total = None
        for k, weight in enumerate(TAPS):
            term = (at(row0 + 2 * q - k) + at(row0 + 2 * q + 1 + k)) * weight
            total = term if total is None else total + term
        results.append(total)
    return results


def halves(value):
    high = value.astype(jnp.bfloat16)
    return high, (value - high.astype(jnp.float32)).astype(jnp.bfloat16)


def split_columns(parts):
    count = len(parts[0])
    highs, lows = [], []
    for q in range(0, count, 2):
        rows = [jnp.concatenate([part[p] for part in parts], axis=1) for p in range(q, min(q + 2, count))]
        high, low = halves(jnp.concatenate(rows, axis=0))
        highs.append(high)
        lows.append(low)
    return jnp.concatenate(highs, axis=0), jnp.concatenate(lows, axis=0)


def dot(left, right):
    return jnp.dot(left, right, preferred_element_type=jnp.float32)


def add_tiles(slot_hbm, tiles_ref, weight_ref, patch_ref, canvas_ref, x_ref, v_ref, w_ref, p_ref, slot_ref, list_ref, sem, wsem, outer):
    def copies(s, i):
        return [
            pltpu.make_async_copy(
                tiles_ref.at[s, :, :, pl.ds(128 * b, 128)], x_ref.at[i, :, b, pl.ds(XPAD, TILE), :], sem.at[i, b]
            )
            for b in range(2)
        ]

    loads = [pltpu.make_async_copy(weight_ref, w_ref, wsem.at[0]), pltpu.make_async_copy(patch_ref, p_ref, wsem.at[1])]
    slots = pltpu.make_async_copy(slot_hbm, slot_ref, wsem.at[2])
    slots.start()
    zero_pad = jnp.zeros((XPAD, 128), jnp.float32)

    def clear_pad(i, carry):
        for c in range(3):
            for b in range(2):
                x_ref[i, c, b, 0:XPAD, :] = zero_pad
                x_ref[i, c, b, XPAD + TILE : 2 * XPAD + TILE, :] = zero_pad
        return carry

    lax.fori_loop(0, 8, clear_pad, 0)
    slots.wait()
    count = jnp.int32(0)
    places = [slot_ref[0, s] for s in range(SLOTS)]
    at_edge = [(place >= 0) & (((place >> 2) == 0) | ((place >> 2) == BR - 1)) for place in places]
    in_middle = [((place >> 2) == 1) | ((place >> 2) == 2) for place in places]
    edges = jnp.int32(0)
    for flag in at_edge:
        edges = edges + flag.astype(jnp.int32)
    spare = QUOTA - edges

    def take(s, wanted, count):
        @pl.when(wanted)
        def _():
            list_ref[count] = s
            for copy in copies(s, count):
                copy.start()

        return count + wanted.astype(jnp.int32)

    if outer:
        for s in range(SLOTS):
            count = take(s, at_edge[s], count)
            if s == 3:
                for copy in loads:
                    copy.start()
    seen = jnp.int32(0)
    for s in range(SLOTS):
        wanted = in_middle[s] & ((seen < spare) if outer else (seen >= spare))
        count = take(s, wanted, count)
        seen = seen + in_middle[s].astype(jnp.int32)
        if s == 3 and not outer:
            for copy in loads:
                copy.start()

    clear_canvas(canvas_ref, ROWS if outer else INNER)
    for copy in loads:
        copy.wait()

    lane = lax.broadcasted_iota(jnp.int32, (1, 128), 1)
    is_left = lane >= 64
    steps = PATCH // 8

    def arrive(i):
        for copy in copies(list_ref[i], i):
            copy.wait()

    def vertical(i):
        for c in range(3):
            parts = [
                fir(lambda t, b=b: x_ref[i, c, b, pl.ds(t, 8, stride=2 * steps), :], steps, XPAD - 16) for b in range(2)
            ]
            v_ref[0, c], v_ref[1, c] = split_columns(parts)

    def horizontal(i):
        place = slot_ref[0, list_ref[i]]
        tile_row = place >> 2
        tile_col = place & 3
        blocks = (tile_col, jnp.where(tile_col == 0, 4, tile_col - 1), tile_col + 1)
        row0 = pl.multiple_of(tile_row * 128 + (8 if outer else -120), 8)

        def add(c, rows, values):
            olds = [[canvas_ref[c, block, r, :] for r in rows] for block in blocks]
            for block, old, new in zip(blocks, olds, values):
                for r, first, second in zip(rows, old, new):
                    canvas_ref[c, block, r, :] = first + second

        for r in range(0, PATCH, 48):
            values = [[p_ref[k, r + t : r + t + 8, :] for t in range(0, 48, 8)] for k in range(3)]
            add(3, [pl.ds(row0 + r + t, 8) for t in range(0, 48, 8)], values)
        for c in range(3):
            first = dot(v_ref[0, c], w_ref[0])
            second = dot(v_ref[1, c], w_ref[1])
            third = dot(v_ref[0, c], w_ref[2])
            main = first[:, :128] + first[:, 128:] + second[:, :128]
            spill = second[:, 128:] + third[:, :128] + third[:, 128:]
            for q0 in range(0, steps, 6):
                mains = [main[8 * q : 8 * q + 8] for q in range(q0, q0 + 6)]
                spills = [spill[8 * q : 8 * q + 8] for q in range(q0, q0 + 6)]
                values = (mains, [jnp.where(is_left, v, 0.0) for v in spills], [jnp.where(is_left, 0.0, v) for v in spills])
                add(c, [pl.ds(row0 + q, 8, stride=steps) for q in range(q0, q0 + 6)], values)

    @pl.when(count > 0)
    def _():
        arrive(0)
        vertical(0)

        def step(i, carry):
            arrive(i)
            horizontal(i - 1)
            vertical(i)
            return carry

        lax.fori_loop(1, count, step, 0)
        horizontal(count - 1)


def clear_canvas(canvas_ref, count):
    zero_rows = jnp.zeros((count // 2, 128), jnp.float32)

    def clear(i, carry):
        c = i // 5
        b = i % 5
        canvas_ref[c, b, 0 : count // 2, :] = zero_rows
        canvas_ref[c, b, count // 2 : count, :] = zero_rows
        return carry

    lax.fori_loop(0, 20, clear, 0)


def outer_kernel(slot_ref, tiles_ref, weight_ref, patch_ref, canvas_ref, up_ref, down_ref, *scratch):
    add_tiles(slot_ref, tiles_ref, weight_ref, patch_ref, canvas_ref, *scratch, True)
    for c in range(4):
        for b in range(5):
            up_ref[c, b] = canvas_ref[c, b, 8:32, :]
            down_ref[c, b] = canvas_ref[c, b, 512:536, :]


def inner_kernel(slot_ref, tiles_ref, weight_ref, patch_ref, canvas_ref, *scratch):
    add_tiles(slot_ref, tiles_ref, weight_ref, patch_ref, canvas_ref, *scratch, False)


def canvas_rows(outer_ref, inner_ref, c, b, row, n, kind):
    value = outer_ref[c, b, pl.ds(row, n), :]
    return value + inner_ref[c, b, pl.ds(row - 128, n), :] if kind else value


KINDS = ((0, 128, 0), (128, 416, 1), (416, ROWS, 0))


def pack_kernel(outer_ref, inner_ref, above_any, below_any, left_ref, right_ref, top_ref, bottom_ref, band_ref, sem):
    bands = [pltpu.make_async_copy(ref, band_ref.at[k], sem.at[k]) for k, ref in enumerate((above_any, below_any))]
    for copy in bands:
        copy.start()
    lane = lax.broadcasted_iota(jnp.int32, (1, 128), 1)
    is_left = lane >= 64

    def rows_of(c, b, start):
        stop = min(start + PACK, ROWS)
        pieces = []
        for low, high, kind in KINDS:
            first, last = max(low, start), min(high, stop)
            if first < last:
                pieces.append(canvas_rows(outer_ref, inner_ref, c, b, first, last - first, kind))
        value = jnp.concatenate(pieces, axis=0) if len(pieces) > 1 else pieces[0]
        if start == 0:
            value = jnp.concatenate([top_ref[c, b], value[TOP:]], axis=0)
        if stop == ROWS:
            value = jnp.concatenate([value[:-TOP], bottom_ref[c, b]], axis=0)
        return value

    def packed(c, block, first, groups, start):
        for g in groups:
            edge, own = rows_of(c, 4, g * PACK), rows_of(c, block, g * PACK)
            band = jnp.where(is_left, edge, own) if block == 0 else jnp.where(is_left, own, edge)
            band = pltpu.roll(band, (first + BAND * g) % 128, 1)
            if start is None:
                start = band
                continue
            rows = band.shape[0]
            mask = (lane >= BAND * g) & (lane < BAND * (g + 1))
            head = jnp.where(mask, band, start[:rows])
            start = head if rows == PACK else jnp.concatenate([head, start[rows:]], axis=0)
        return start

    sides = ((left_ref, 0, 3), (right_ref, 3, 15))
    for c in range(4):
        for out_ref, block, first in sides:
            out_ref[c] = packed(c, block, first, range(1, GROUPS - 1), None)
    for copy in bands:
        copy.wait()
    for c in range(4):
        for b in range(5):
            top_ref[c, b] = outer_ref[c, b, 0:TOP, :] + band_ref[0, c, b]
            bottom_ref[c, b] = outer_ref[c, b, ROWS - TOP : ROWS, :] + band_ref[1, c, b]
    for c in range(4):
        for out_ref, block, first in sides:
            out_ref[c] = packed(c, block, first, (0, GROUPS - 1), out_ref[c])


def finish(linear):
    weight = linear[3]
    scale = 1.0 / jnp.maximum(weight, WEIGHT_FLOOR)
    opacity = jnp.clip(weight, 0.0, 1.0)
    colour = [linear[c] * scale for c in range(3)]
    return colour + [opacity], [value * opacity for value in colour] + [opacity]


def neighbours():
    row, col = lax.axis_index("row"), lax.axis_index("col")
    found = (row > 0, row < lax.axis_size("row") - 1, col > 0, col < lax.axis_size("col") - 1)
    return [jnp.where(flag, 1.0, 0.0).astype(jnp.float32) for flag in found]


def level_one_rows(top_ref, bottom_ref, finish_one, copies):
    has_above, has_below, _, _ = neighbours()

    def run(low, high, kind):
        def body(i, carry):
            row = pl.multiple_of(low + 16 * i, 16)
            finish_one(row, 16, None, 0, None, row - 16, kind)
            return carry

        lax.fori_loop(0, (high - low) // 16, body, 0)

    finish_one(0, 16, top_ref, 0, has_above, None, 0)
    finish_one(16, 8, top_ref, 16, None, 0, 0)
    finish_one(24, 8, None, 0, None, 8, 0)
    run(32, 128, 0)
    run(128, 272, 1)
    for copy in copies[0]:
        copy.start()
    run(272, 416, 1)
    run(416, 512, 0)
    finish_one(512, 8, None, 0, None, 496, 0)
    finish_one(520, 8, bottom_ref, 0, None, 504, 0)
    for copy in copies[1]:
        copy.start()
    finish_one(528, 16, bottom_ref, 8, has_below, None, 0)


def clear_carried(carried_ref, blocks):
    zero_pad = jnp.zeros((CPAD, 128), jnp.float32)
    for c in range(4):
        for b in range(blocks):
            carried_ref[c, b, 0:CPAD, :] = zero_pad
            carried_ref[c, b, CPAD + ROWS : CROWS, :] = zero_pad


STEPS2 = ROWS2 // 8
STEPS3 = 17


def middle_kernel(outer_ref, inner_ref, top_ref, bottom_ref, own_hbm, one_out, part_ref, carried_ref, one_ref, own_ref, sem):
    load = pltpu.make_async_copy(own_hbm, own_ref, sem.at[2])
    load.start()
    clear_carried(carried_ref, 2)

    def finish_one(row, n, band, band_row, mask, out_row, kind):
        for b in range(2):
            linear = []
            for c in range(4):
                if band is None:
                    value = canvas_rows(outer_ref, inner_ref, c, b + 1, row, n, kind)
                else:
                    value = band[c, b + 1, pl.ds(band_row, n), :]
                if mask is not None:
                    value = value * mask
                linear.append(value)
            shown, carried = finish(linear)
            for c in range(4):
                if out_row is not None:
                    one_ref[c, pl.ds(out_row, n), 128 * b : 128 * b + 128] = shown[c]
                carried_ref[c, b, pl.ds(row + CPAD, n), :] = carried[c]

    copies = [
        [
            pltpu.make_async_copy(
                one_ref.at[:, pl.ds(256 * q, 256), :], one_out.at[:, pl.ds(256 * q, 256), pl.ds(128, 256)], sem.at[q]
            )
        ]
        for q in range(2)
    ]
    level_one_rows(top_ref, bottom_ref, finish_one, copies)
    load.wait()

    def reduce_two(c, carry):
        parts = [
            fir(lambda t, b=b: carried_ref[c, b, pl.ds(t, 8, stride=2 * STEPS2), :], STEPS2, CPAD) for b in range(2)
        ]
        high, low = split_columns(parts)
        own = dot(high, own_ref[0]) + dot(high, own_ref[1]) + dot(low, own_ref[0])
        part_ref[c, 0] = own[:, :128]
        part_ref[c, 1] = own[:, 128:]
        return carry

    for c in range(4):
        reduce_two(c, 0)
    for pair in copies:
        for copy in pair:
            copy.wait()


def levels_kernel(
    outer_ref, inner_ref, top_ref, bottom_ref, from_left_ref, from_right_ref, part_ref, own_hbm, one_in,
    one_out, two_out, three_out,
    add_ref, carried_ref, linear_ref, carried2_ref, one_ref, two_ref, three_stage, w_ref, sem,
):
    load = pltpu.make_async_copy(own_hbm, w_ref, sem.at[6])
    load.start()
    has_above, has_below, has_left, has_right = neighbours()
    lane = lax.broadcasted_iota(jnp.int32, (1, 128), 1)
    is_left = lane >= 64
    edge_mask = jnp.where(is_left, has_left, has_right)
    clear_carried(carried_ref, 3)
    for c in range(4):
        for b in range(3):
            carried2_ref[c, b, ROWS2 : ROWS2 + 16, :] = jnp.zeros((16, 128), jnp.float32)

    from_left_lanes = (lane >= 113) | (lane < 3)
    from_right_lanes = (lane >= 125) | (lane < 15)
    for c in range(4):
        for side, ref, first, lanes in ((0, from_left_ref, 15, from_left_lanes), (1, from_right_ref, 3, from_right_lanes)):
            for g in range(GROUPS):
                start, stop = g * PACK, min(g * PACK + PACK, ROWS)
                band = pltpu.roll(ref[c, 0 : stop - start, :], (-first - BAND * g) % 128, 1)
                add_ref[side, c, start:stop, :] = jnp.where(lanes, band, 0.0)

    def finish_one(row, n, band, band_row, mask, out_row, kind):
        rows = pl.ds(row, n)
        for b, block in enumerate((0, 3, 4)):
            linear = []
            for c in range(4):
                if band is None:
                    value = canvas_rows(outer_ref, inner_ref, c, block, row, n, kind)
                else:
                    value = band[c, block, pl.ds(band_row, n), :]
                if b == 0:
                    value = value + jnp.where(is_left, 0.0, add_ref[0, c, rows, :])
                if b == 1:
                    value = value + jnp.where(is_left, add_ref[1, c, rows, :], 0.0)
                if b == 2:
                    value = value + jnp.where(is_left, add_ref[0, c, rows, :], add_ref[1, c, rows, :])
                    value = value * edge_mask
                if mask is not None:
                    value = value * mask
                linear.append(value)
            shown, carried = finish(linear)
            for c in range(4):
                if b < 2 and out_row is not None:
                    one_ref[b, c, pl.ds(out_row, n), :] = shown[c]
                carried_ref[c, b, pl.ds(row + CPAD, n), :] = carried[c]

    copies = [
        [
            pltpu.make_async_copy(
                one_ref.at[b, :, pl.ds(256 * q, 256), :],
                one_out.at[:, pl.ds(256 * q, 256), pl.ds(384 * b, 128)],
                sem.at[2 * q + b],
            )
            for b in range(2)
        ]
        for q in range(2)
    ]
    level_one_rows(top_ref, bottom_ref, finish_one, copies)
    load.wait()

    def reduce_two(c, carry):
        parts = [
            fir(lambda t, b=b: carried_ref[c, b, pl.ds(t, 8, stride=2 * STEPS2), :], STEPS2, CPAD) for b in range(3)
        ]
        high, low = split_columns(parts)
        ends, ends_low = high[:, :256], low[:, :256]
        both = jnp.concatenate([high[:, 256:], low[:, 256:]], axis=1)
        own = dot(ends, w_ref[0]) + dot(ends, w_ref[1]) + dot(ends_low, w_ref[0])
        own = own + dot(both, w_ref[2]) + dot(high[:, 256:], w_ref[3, :128, :])
        edge = dot(ends, w_ref[4]) + dot(both, w_ref[5])
        edge = edge[:, :128] + edge[:, 128:] + dot(ends_low, w_ref[4, :, :128])
        own_left = own[:, :128] + part_ref[c, 0]
        own_right = own[:, 128:] + part_ref[c, 1]
        for q in range(STEPS2):
            rows = pl.ds(q, 8, stride=STEPS2)
            linear_ref[c, 0, rows, :] = own_left[8 * q : 8 * q + 8]
            linear_ref[c, 1, rows, :] = own_right[8 * q : 8 * q + 8]
            linear_ref[c, 2, rows, :] = edge[8 * q : 8 * q + 8]
        return carry

    for c in range(4):
        reduce_two(c, 0)

    def finish_two(row, n, mask, out_row):
        rows = pl.ds(row, n)
        for b in range(3):
            linear = []
            for c in range(4):
                value = linear_ref[c, b, rows, :]
                if b == 2:
                    value = value * edge_mask
                if mask is not None:
                    value = value * mask
                linear.append(value)
            shown, carried = finish(linear)
            for c in range(4):
                if b < 2 and out_row is not None:
                    two_ref[c, pl.ds(out_row, n), 128 * b : 128 * b + 128] = shown[c]
                carried2_ref[c, b, rows, :] = carried[c]

    finish_two(0, 8, has_above, None)

    def body_two(i, carry):
        out_row = pl.multiple_of(16 * i, 16)
        finish_two(out_row + 8, 16, None, out_row)
        return carry

    lax.fori_loop(0, 16, body_two, 0)
    finish_two(264, 8, has_below, None)
    two_copy = pltpu.make_async_copy(two_ref, two_out, sem.at[4])
    two_copy.start()

    def reduce_three(c, carry):
        parts = [
            fir(lambda t, b=b: carried2_ref[c, b, pl.ds(t, 8, stride=2 * STEPS3), :], STEPS3, 8) for b in range(3)
        ]
        high, low = split_columns(parts)
        both = jnp.concatenate([high[:, 256:], low[:, 256:]], axis=1)
        total = dot(high[:, :256], w_ref[6]) + dot(both, w_ref[7])
        total = total[:, :128] + total[:, 128:] + dot(low[:, :256], w_ref[6, :, :128])
        for q in range(STEPS3):
            linear_ref[c, 0, pl.ds(q, 8, stride=STEPS3), :] = total[8 * q : 8 * q + 8]
        return carry

    for c in range(4):
        reduce_three(c, 0)
    for row in range(0, 128, 16):
        shown, _ = finish([linear_ref[c, 0, row : row + 16, :] for c in range(4)])
        for c in range(4):
            three_stage[c, row : row + 16, :] = shown[c]
    three_copy = pltpu.make_async_copy(three_stage, three_out, sem.at[5])
    three_copy.start()
    for pair in copies:
        for copy in pair:
            copy.wait()
    two_copy.wait()
    three_copy.wait()


VMEM = pl.BlockSpec(memory_space=pltpu.VMEM)
HBM = pl.BlockSpec(memory_space=pltpu.HBM)
ANY = pl.BlockSpec(memory_space=pl.ANY)
F32 = jnp.float32
BF16 = jnp.bfloat16


def params(mib):
    return pltpu.CompilerParams(vmem_limit_bytes=mib << 20)


def shifted(value, axis, steps):
    count = lax.axis_size(axis)
    pairs = [(i, i + steps) for i in range(count) if 0 <= i + steps < count]
    return lax.ppermute(value, axis, pairs)


def per_device(tiles, slot_tile):
    shape = jax.ShapeDtypeStruct
    band_shape = pltpu.VMEM((4, 5, TOP, 128), F32)
    pack_shape = pltpu.VMEM((4, PACK, 128), F32)
    in_hbm = lambda value: pltpu.with_memory_space_constraint(value, pltpu.HBM)
    weights, patch = in_hbm(jnp.asarray(tile_weights())), in_hbm(jnp.asarray(opacity_patch()))
    data, slots = in_hbm(tiles[0]), in_hbm(slot_tile)
    scratch = [
        pltpu.VMEM((8, 3, 2, TILE + 2 * XPAD, 128), F32),
        pltpu.VMEM((2, 3, PATCH, 256), BF16),
        pltpu.VMEM((3, 256, 256), BF16),
        pltpu.VMEM((3, PATCH, 128), F32),
        pltpu.SMEM((1, SLOTS), jnp.int32),
        pltpu.SMEM((SLOTS,), jnp.int32),
        pltpu.SemaphoreType.DMA((8, 2)),
        pltpu.SemaphoreType.DMA((3,)),
    ]
    outer, up, down = pl.pallas_call(
        outer_kernel,
        name="outer",
        out_shape=(pltpu.VMEM((4, 5, ROWS, 128), F32), band_shape, band_shape),
        in_specs=[HBM] * 4,
        out_specs=(VMEM, VMEM, VMEM),
        scratch_shapes=scratch,
        compiler_params=params(30),
    )(slots, data, weights, patch)
    below = shifted(up, "row", -1)
    above = shifted(down, "row", 1)
    inner = pl.pallas_call(
        inner_kernel,
        name="inner",
        out_shape=pltpu.VMEM((4, 5, INNER, 128), F32),
        in_specs=[HBM] * 4,
        out_specs=VMEM,
        scratch_shapes=scratch,
        cost_estimate=pl.CostEstimate(flops=4_000_000_000, bytes_accessed=4_000_000, transcendentals=0),
        compiler_params=params(30),
    )(slots, data, weights, patch)
    to_left, to_right, top, bottom = pl.pallas_call(
        pack_kernel,
        name="pack",
        out_shape=(pack_shape, pack_shape, band_shape, band_shape),
        in_specs=[VMEM, VMEM, ANY, ANY],
        out_specs=(VMEM,) * 4,
        scratch_shapes=[pltpu.VMEM((2, 4, 5, TOP, 128), F32), pltpu.SemaphoreType.DMA((2,))],
        compiler_params=params(20),
    )(outer, inner, above, below)
    from_right = shifted(to_left, "col", -1)
    from_left = shifted(to_right, "col", 1)
    middle, rest = level_two_weights()
    level_one, part = pl.pallas_call(
        middle_kernel,
        name="middle",
        out_shape=(shape((4, 512, 512), F32), pltpu.VMEM((4, 2, ROWS2, 128), F32)),
        in_specs=[VMEM, VMEM, VMEM, VMEM, HBM],
        out_specs=(HBM, VMEM),
        scratch_shapes=[
            pltpu.VMEM((4, 2, CROWS, 128), F32),
            pltpu.VMEM((4, 512, 256), F32),
            pltpu.VMEM((2, 256, 256), BF16),
            pltpu.SemaphoreType.DMA((3,)),
        ],
        cost_estimate=pl.CostEstimate(flops=4_000_000_000, bytes_accessed=4_000_000, transcendentals=0),
        compiler_params=params(30),
    )(outer, inner, top, bottom, in_hbm(jnp.asarray(middle)))
    return pl.pallas_call(
        levels_kernel,
        name="levels",
        out_shape=(shape((4, 512, 512), F32), shape((4, 256, 256), F32), shape((4, 128, 128), F32)),
        in_specs=[VMEM] * 7 + [HBM, HBM],
        out_specs=(HBM, HBM, HBM),
        scratch_shapes=[
            pltpu.VMEM((2, 4, ROWS, 128), F32),
            pltpu.VMEM((4, 3, CROWS, 128), F32),
            pltpu.VMEM((4, 3, ROWS2, 128), F32),
            pltpu.VMEM((4, 3, ROWS2 + 16, 128), F32),
            pltpu.VMEM((2, 4, 512, 128), F32),
            pltpu.VMEM((4, 256, 256), F32),
            pltpu.VMEM((4, 128, 128), F32),
            pltpu.VMEM((8, 256, 256), BF16),
            pltpu.SemaphoreType.DMA((7,)),
        ],
        input_output_aliases={8: 0},
        compiler_params=params(30),
    )(outer, inner, top, bottom, from_left, from_right, part, in_hbm(jnp.asarray(rest)), level_one)


def solution(mesh):
    placed = (P("row", "col", None, None, None), P("row", "col"))
    return jax.shard_map(
        per_device,
        mesh=mesh,
        in_specs=placed,
        out_specs=(P(None, "row", "col"), P(None, "row", "col"), P(None, "row", "col")),
        check_vma=False,
    )
```

```python
import jax
import jax.numpy as jnp
import numpy as np
from jax import lax
from jax.experimental import pallas as pl
from jax.experimental.pallas import tpu as pltpu
from jax.sharding import PartitionSpec as P

BR = 4
BC = 4
SLOTS = 12
TILE = 256
WEIGHT_FLOOR = 0.25

ROWS = 544
INNER = 288
QUOTA = 8
PATCH = 144
TOP = 24
BAND = 18
GROUPS = 7
PACK = 80
FLAG_ROW = 64
FLAG_LANE = 108
XPAD = 24
CPAD = 8
CROWS = 560
ROWS2 = 272


def lanczos(t):
    return np.where(np.abs(t) < 3.0, np.sinc(t) * np.sinc(t / 3.0), 0.0)


SUPPORT = lanczos((np.arange(-5, 7) - 0.5) / 2.0)
NORM = SUPPORT.sum()
TAPS = [float(np.float32(v / NORM)) for v in SUPPORT[5::-1]]


def taper(d):
    return (lanczos((d - 0.5) / 2.0) / NORM).astype(np.float32)


def split(matrix):
    high = matrix.astype(jnp.bfloat16)
    low = (matrix - high.astype(np.float32)).astype(jnp.bfloat16)
    return high, low


def tile_weights():
    x = np.arange(TILE)[:, None]
    lane = np.arange(128)[None, :]
    main = taper(x - 2 * lane)
    spill = np.where(lane < 8, taper(x - 2 * (lane + 128)), np.where(lane >= 120, taper(x - 2 * (lane - 128)), 0.0))
    spill = spill.astype(np.float32)
    mh, ml = split(main)
    sh, sl = split(spill)
    return np.stack([np.concatenate(pair, axis=1) for pair in ((mh, ml), (mh, sh), (sh, sl))])


def opacity_patch():
    x = np.arange(TILE)[None, :]
    rows = taper(x - 2 * np.arange(-8, PATCH - 8)[:, None]).sum(axis=1, dtype=np.float64)
    main = taper(x - 2 * np.arange(128)[:, None]).sum(axis=1, dtype=np.float64)
    lane = np.arange(128)
    right = taper(x - 2 * (lane[:, None] + 128)).sum(axis=1, dtype=np.float64)
    left = taper(x - 2 * (lane[:, None] - 128)).sum(axis=1, dtype=np.float64)
    cols = np.stack([main, np.where(lane >= 64, left, 0.0), np.where(lane < 64, right, 0.0)])
    return (cols[:, None, :] * rows[None, :, None]).astype(np.float32)


def band_opacity():
    main, left, right = opacity_patch()
    lane = np.arange(128)
    from_left = np.where(lane >= 113, main, np.where(lane < 3, right, 0.0))
    from_right = np.where(lane < 15, main, np.where(lane >= 125, left, 0.0))
    return np.stack([from_left, from_right]).astype(np.float32)


def wide_weights(own):
    edge = np.arange(128)
    cols_in = np.concatenate([np.arange(own), np.where(edge < 64, own + edge, edge - 128)])[:, None]
    cols_own = np.arange(own // 2)[None, :]
    cols_edge = np.where(edge < 64, own // 2 + edge, edge - 128)[None, :]
    return taper(cols_in - 2 * cols_own), taper(cols_in - 2 * cols_edge)


def level_two_weights():
    oh, ol = split(wide_weights(512)[0])
    eh, el = split(wide_weights(512)[1])
    th, tl = split(wide_weights(256)[0])
    zero = np.zeros((128, 128), eh.dtype)
    ends = lambda m: np.concatenate([m[:128], m[384:512]])
    beside = lambda *parts: np.concatenate(parts, axis=1)
    rest = [
        ends(oh),
        ends(ol),
        np.concatenate([oh[512:], oh[512:]]),
        np.concatenate([ol[512:], ol[512:]]),
        beside(ends(eh), ends(el)),
        np.concatenate([beside(eh[512:], el[512:]), beside(eh[512:], zero)]),
        beside(th[:256], tl[:256]),
        np.concatenate([beside(th[256:], tl[256:]), beside(th[256:], zero)]),
    ]
    return np.stack([oh[128:384], ol[128:384]]), np.stack(rest)


def fir(load, count, row0):
    rows = {}

    def at(t):
        if t not in rows:
            rows[t] = load(t)
        return rows[t]

    results = []
    for q in range(count):
        total = None
        for k, weight in enumerate(TAPS):
            term = (at(row0 + 2 * q - k) + at(row0 + 2 * q + 1 + k)) * weight
            total = term if total is None else total + term
        results.append(total)
    return results


def halves(value):
    high = value.astype(jnp.bfloat16)
    return high, (value - high.astype(jnp.float32)).astype(jnp.bfloat16)


def split_columns(parts):
    count = len(parts[0])
    highs, lows = [], []
    for q in range(0, count, 2):
        rows = [jnp.concatenate([part[p] for part in parts], axis=1) for p in range(q, min(q + 2, count))]
        high, low = halves(jnp.concatenate(rows, axis=0))
        highs.append(high)
        lows.append(low)
    return jnp.concatenate(highs, axis=0), jnp.concatenate(lows, axis=0)


def dot(left, right):
    return jnp.dot(left, right, preferred_element_type=jnp.float32)


def add_tiles(slot_hbm, tiles_ref, weight_ref, patch_ref, canvas_ref, x_ref, v_ref, w_ref, p_ref, slot_ref, list_ref, sem, wsem, outer):
    def copies(s, i):
        return [
            pltpu.make_async_copy(
                tiles_ref.at[s, :, :, pl.ds(128 * b, 128)], x_ref.at[i, :, b, pl.ds(XPAD, TILE), :], sem.at[i, b]
            )
            for b in range(2)
        ]

    loads = [pltpu.make_async_copy(weight_ref, w_ref, wsem.at[0]), pltpu.make_async_copy(patch_ref, p_ref, wsem.at[1])]
    slots = pltpu.make_async_copy(slot_hbm, slot_ref, wsem.at[2])
    slots.start()
    zero_pad = jnp.zeros((XPAD, 128), jnp.float32)

    def clear_pad(i, carry):
        for c in range(3):
            for b in range(2):
                x_ref[i, c, b, 0:XPAD, :] = zero_pad
                x_ref[i, c, b, XPAD + TILE : 2 * XPAD + TILE, :] = zero_pad
        return carry

    lax.fori_loop(0, 8, clear_pad, 0)
    slots.wait()
    count = jnp.int32(0)
    places = [slot_ref[0, s] for s in range(SLOTS)]
    at_edge = [(place >= 0) & (((place >> 2) == 0) | ((place >> 2) == BR - 1)) for place in places]
    in_middle = [((place >> 2) == 1) | ((place >> 2) == 2) for place in places]
    edges = jnp.int32(0)
    for flag in at_edge:
        edges = edges + flag.astype(jnp.int32)
    spare = QUOTA - edges

    def take(s, wanted, count):
        @pl.when(wanted)
        def _():
            list_ref[count] = s
            for copy in copies(s, count):
                copy.start()

        return count + wanted.astype(jnp.int32)

    if outer:
        for s in range(SLOTS):
            count = take(s, at_edge[s], count)
            if s == 3:
                for copy in loads:
                    copy.start()
    seen = jnp.int32(0)
    for s in range(SLOTS):
        wanted = in_middle[s] & ((seen < spare) if outer else (seen >= spare))
        count = take(s, wanted, count)
        seen = seen + in_middle[s].astype(jnp.int32)
        if s == 3 and not outer:
            for copy in loads:
                copy.start()

    clear_canvas(canvas_ref, ROWS if outer else INNER)
    for copy in loads:
        copy.wait()

    lane = lax.broadcasted_iota(jnp.int32, (1, 128), 1)
    is_left = lane >= 64
    steps = PATCH // 8

    def arrive(i):
        for copy in copies(list_ref[i], i):
            copy.wait()

    def vertical(i):
        for c in range(3):
            parts = [
                fir(lambda t, b=b: x_ref[i, c, b, pl.ds(t, 8, stride=2 * steps), :], steps, XPAD - 16) for b in range(2)
            ]
            v_ref[0, c], v_ref[1, c] = split_columns(parts)

    def horizontal(i):
        place = slot_ref[0, list_ref[i]]
        tile_row = place >> 2
        tile_col = place & 3
        blocks = (tile_col, jnp.where(tile_col == 0, 4, tile_col - 1), tile_col + 1)
        row0 = pl.multiple_of(tile_row * 128 + (8 if outer else -120), 8)

        def add(c, rows, values):
            olds = [[canvas_ref[c, block, r, :] for r in rows] for block in blocks]
            for block, old, new in zip(blocks, olds, values):
                for r, first, second in zip(rows, old, new):
                    canvas_ref[c, block, r, :] = first + second

        for r in range(0, PATCH, 48):
            values = [[p_ref[k, r + t : r + t + 8, :] for t in range(0, 48, 8)] for k in range(3)]
            add(3, [pl.ds(row0 + r + t, 8) for t in range(0, 48, 8)], values)
        for c in range(3):
            first = dot(v_ref[0, c], w_ref[0])
            second = dot(v_ref[1, c], w_ref[1])
            third = dot(v_ref[0, c], w_ref[2])
            main = first[:, :128] + first[:, 128:] + second[:, :128]
            spill = second[:, 128:] + third[:, :128] + third[:, 128:]
            for q0 in range(0, steps, 6):
                mains = [main[8 * q : 8 * q + 8] for q in range(q0, q0 + 6)]
                spills = [spill[8 * q : 8 * q + 8] for q in range(q0, q0 + 6)]
                values = (mains, [jnp.where(is_left, v, 0.0) for v in spills], [jnp.where(is_left, 0.0, v) for v in spills])
                add(c, [pl.ds(row0 + q, 8, stride=steps) for q in range(q0, q0 + 6)], values)

    @pl.when(count > 0)
    def _():
        arrive(0)
        vertical(0)

        def step(i, carry):
            arrive(i)
            horizontal(i - 1)
            vertical(i)
            return carry

        lax.fori_loop(1, count, step, 0)
        horizontal(count - 1)


def clear_canvas(canvas_ref, count):
    zero_rows = jnp.zeros((count // 2, 128), jnp.float32)

    def clear(i, carry):
        c = i // 5
        b = i % 5
        canvas_ref[c, b, 0 : count // 2, :] = zero_rows
        canvas_ref[c, b, count // 2 : count, :] = zero_rows
        return carry

    lax.fori_loop(0, 20, clear, 0)


def outer_kernel(slot_ref, tiles_ref, weight_ref, patch_ref, canvas_ref, up_ref, down_ref, *scratch):
    add_tiles(slot_ref, tiles_ref, weight_ref, patch_ref, canvas_ref, *scratch, True)
    for c in range(4):
        for b in range(5):
            up_ref[c, b] = canvas_ref[c, b, 8:32, :]
            down_ref[c, b] = canvas_ref[c, b, 512:536, :]


def inner_kernel(slot_ref, tiles_ref, weight_ref, patch_ref, canvas_ref, *scratch):
    add_tiles(slot_ref, tiles_ref, weight_ref, patch_ref, canvas_ref, *scratch, False)


def canvas_rows(outer_ref, inner_ref, c, b, row, n, kind):
    value = outer_ref[c, b, pl.ds(row, n), :]
    return value + inner_ref[c, b, pl.ds(row - 128, n), :] if kind else value


KINDS = ((0, 128, 0), (128, 416, 1), (416, ROWS, 0))


def pack_kernel(outer_ref, inner_ref, above_any, below_any, left_ref, right_ref, top_ref, bottom_ref, band_ref, sem):
    bands = [pltpu.make_async_copy(ref, band_ref.at[k], sem.at[k]) for k, ref in enumerate((above_any, below_any))]
    for copy in bands:
        copy.start()
    lane = lax.broadcasted_iota(jnp.int32, (1, 128), 1)
    is_left = lane >= 64

    def rows_of(c, b, start):
        stop = min(start + PACK, ROWS)
        pieces = []
        for low, high, kind in KINDS:
            first, last = max(low, start), min(high, stop)
            if first < last:
                pieces.append(canvas_rows(outer_ref, inner_ref, c, b, first, last - first, kind))
        value = jnp.concatenate(pieces, axis=0) if len(pieces) > 1 else pieces[0]
        if start == 0:
            value = jnp.concatenate([top_ref[c, b], value[TOP:]], axis=0)
        if stop == ROWS:
            value = jnp.concatenate([value[:-TOP], bottom_ref[c, b]], axis=0)
        return value

    def packed(c, block, first, groups, start):
        for g in groups:
            edge, own = rows_of(c, 4, g * PACK), rows_of(c, block, g * PACK)
            band = jnp.where(is_left, edge, own) if block == 0 else jnp.where(is_left, own, edge)
            band = pltpu.roll(band, (first + BAND * g) % 128, 1)
            if start is None:
                start = band
                continue
            rows = band.shape[0]
            mask = (lane >= BAND * g) & (lane < BAND * (g + 1))
            head = jnp.where(mask, band, start[:rows])
            start = head if rows == PACK else jnp.concatenate([head, start[rows:]], axis=0)
        return start

    sides = ((left_ref, 0, 3), (right_ref, 3, 15))
    for c in range(3):
        for out_ref, block, first in sides:
            out_ref[c] = packed(c, block, first, range(1, GROUPS - 1), None)
    for copy in bands:
        copy.wait()
    for c in range(4):
        for b in range(5):
            top_ref[c, b] = outer_ref[c, b, 0:TOP, :] + band_ref[0, c, b]
            bottom_ref[c, b] = outer_ref[c, b, ROWS - TOP : ROWS, :] + band_ref[1, c, b]
    for c in range(3):
        for out_ref, block, first in sides:
            out_ref[c] = packed(c, block, first, (0, GROUPS - 1), out_ref[c])
    for out_ref, block, _ in sides:
        shown = [top_ref[3, block, 6:7, :]]
        for start in (76, 204, 332, 460):
            shown.append(canvas_rows(outer_ref, inner_ref, 3, block, start, 1, 128 <= start < 416))
        shown.append(bottom_ref[3, block, 16:17, :])
        for i, value in enumerate(shown):
            row = slice(FLAG_ROW + i, FLAG_ROW + i + 1)
            out_ref[0, row, :] = jnp.where(lane >= FLAG_LANE, value, out_ref[0, row, :])


def finish(linear):
    weight = linear[3]
    scale = 1.0 / jnp.maximum(weight, WEIGHT_FLOOR)
    opacity = jnp.clip(weight, 0.0, 1.0)
    colour = [linear[c] * scale for c in range(3)]
    return colour + [opacity], [value * opacity for value in colour] + [opacity]


def neighbours():
    row, col = lax.axis_index("row"), lax.axis_index("col")
    found = (row > 0, row < lax.axis_size("row") - 1, col > 0, col < lax.axis_size("col") - 1)
    return [jnp.where(flag, 1.0, 0.0).astype(jnp.float32) for flag in found]


def level_one_rows(top_ref, bottom_ref, finish_one, copies):
    has_above, has_below, _, _ = neighbours()

    def run(low, high, kind):
        def body(i, carry):
            row = pl.multiple_of(low + 16 * i, 16)
            finish_one(row, 16, None, 0, None, row - 16, kind)
            return carry

        lax.fori_loop(0, (high - low) // 16, body, 0)

    finish_one(0, 16, top_ref, 0, has_above, None, 0)
    finish_one(16, 8, top_ref, 16, None, 0, 0)
    finish_one(24, 8, None, 0, None, 8, 0)
    run(32, 128, 0)
    run(128, 272, 1)
    for copy in copies[0]:
        copy.start()
    run(272, 416, 1)
    run(416, 512, 0)
    finish_one(512, 8, None, 0, None, 496, 0)
    finish_one(520, 8, bottom_ref, 0, None, 504, 0)
    for copy in copies[1]:
        copy.start()
    finish_one(528, 16, bottom_ref, 8, has_below, None, 0)


def clear_carried(carried_ref, blocks):
    zero_pad = jnp.zeros((CPAD, 128), jnp.float32)
    for c in range(4):
        for b in range(blocks):
            carried_ref[c, b, 0:CPAD, :] = zero_pad
            carried_ref[c, b, CPAD + ROWS : CROWS, :] = zero_pad


STEPS2 = ROWS2 // 8
STEPS3 = 17


def middle_kernel(outer_ref, inner_ref, top_ref, bottom_ref, own_hbm, table_hbm, one_out, part_ref, table_ref, carried_ref, one_ref, own_ref, sem):
    load = pltpu.make_async_copy(own_hbm, own_ref, sem.at[2])
    load.start()
    table_load = pltpu.make_async_copy(table_hbm, table_ref, sem.at[3])
    table_load.start()
    clear_carried(carried_ref, 2)

    def finish_one(row, n, band, band_row, mask, out_row, kind):
        for b in range(2):
            linear = []
            for c in range(4):
                if band is None:
                    value = canvas_rows(outer_ref, inner_ref, c, b + 1, row, n, kind)
                else:
                    value = band[c, b + 1, pl.ds(band_row, n), :]
                if mask is not None:
                    value = value * mask
                linear.append(value)
            shown, carried = finish(linear)
            for c in range(4):
                if out_row is not None:
                    one_ref[c, pl.ds(out_row, n), 128 * b : 128 * b + 128] = shown[c]
                carried_ref[c, b, pl.ds(row + CPAD, n), :] = carried[c]

    copies = [
        [
            pltpu.make_async_copy(
                one_ref.at[:, pl.ds(256 * q, 256), :], one_out.at[:, pl.ds(256 * q, 256), pl.ds(128, 256)], sem.at[q]
            )
        ]
        for q in range(2)
    ]
    level_one_rows(top_ref, bottom_ref, finish_one, copies)
    load.wait()
    table_load.wait()

    def reduce_two(c, carry):
        parts = [
            fir(lambda t, b=b: carried_ref[c, b, pl.ds(t, 8, stride=2 * STEPS2), :], STEPS2, CPAD) for b in range(2)
        ]
        high, low = split_columns(parts)
        own = dot(high, own_ref[0]) + dot(high, own_ref[1]) + dot(low, own_ref[0])
        part_ref[c, 0] = own[:, :128]
        part_ref[c, 1] = own[:, 128:]
        return carry

    for c in range(4):
        reduce_two(c, 0)
    for pair in copies:
        for copy in pair:
            copy.wait()


def levels_kernel(
    outer_ref, inner_ref, top_ref, bottom_ref, from_left_ref, from_right_ref, part_ref, table_ref, own_hbm, one_in,
    one_out, two_out, three_out,
    add_ref, carried_ref, linear_ref, carried2_ref, one_ref, two_ref, three_stage, w_ref, sem,
):
    load = pltpu.make_async_copy(own_hbm, w_ref, sem.at[6])
    load.start()
    has_above, has_below, has_left, has_right = neighbours()
    lane = lax.broadcasted_iota(jnp.int32, (1, 128), 1)
    is_left = lane >= 64
    edge_mask = jnp.where(is_left, has_left, has_right)
    clear_carried(carried_ref, 3)
    for c in range(4):
        for b in range(3):
            carried2_ref[c, b, ROWS2 : ROWS2 + 16, :] = jnp.zeros((16, 128), jnp.float32)

    from_left_lanes = (lane >= 113) | (lane < 3)
    from_right_lanes = (lane >= 125) | (lane < 15)
    for c in range(3):
        for side, ref, first, lanes in ((0, from_left_ref, 15, from_left_lanes), (1, from_right_ref, 3, from_right_lanes)):
            for g in range(GROUPS):
                start, stop = g * PACK, min(g * PACK + PACK, ROWS)
                band = pltpu.roll(ref[c, 0 : stop - start, :], (-first - BAND * g) % 128, 1)
                add_ref[side, c, start:stop, :] = jnp.where(lanes, band, 0.0)

    for side, ref in ((0, from_left_ref), (1, from_right_ref)):
        flags = [
            jnp.where(ref[0, FLAG_ROW + i : FLAG_ROW + i + 1, FLAG_LANE : FLAG_LANE + 1] > 0.5, 1.0, 0.0) for i in range(6)
        ]
        flags = [jnp.broadcast_to(flag, (8, 128)) for flag in flags]
        for start in range(0, ROWS, 8):
            total = None
            for i in range(6):
                row = start - 128 * (i - 1) - 8
                if 0 <= row < PATCH:
                    term = table_ref[side, row : row + 8, :] * flags[i]
                    total = term if total is None else total + term
            add_ref[side, 3, start : start + 8, :] = total

    def finish_one(row, n, band, band_row, mask, out_row, kind):
        rows = pl.ds(row, n)
        for b, block in enumerate((0, 3, 4)):
            linear = []
            for c in range(4):
                if band is None:
                    value = canvas_rows(outer_ref, inner_ref, c, block, row, n, kind)
                else:
                    value = band[c, block, pl.ds(band_row, n), :]
                if b == 0:
                    value = value + jnp.where(is_left, 0.0, add_ref[0, c, rows, :])
                if b == 1:
                    value = value + jnp.where(is_left, add_ref[1, c, rows, :], 0.0)
                if b == 2:
                    value = value + jnp.where(is_left, add_ref[0, c, rows, :], add_ref[1, c, rows, :])
                    value = value * edge_mask
                if mask is not None:
                    value = value * mask
                linear.append(value)
            shown, carried = finish(linear)
            for c in range(4):
                if b < 2 and out_row is not None:
                    one_ref[b, c, pl.ds(out_row, n), :] = shown[c]
                carried_ref[c, b, pl.ds(row + CPAD, n), :] = carried[c]

    copies = [
        [
            pltpu.make_async_copy(
                one_ref.at[b, :, pl.ds(256 * q, 256), :],
                one_out.at[:, pl.ds(256 * q, 256), pl.ds(384 * b, 128)],
                sem.at[2 * q + b],
            )
            for b in range(2)
        ]
        for q in range(2)
    ]
    level_one_rows(top_ref, bottom_ref, finish_one, copies)
    load.wait()

    def reduce_two(c, carry):
        parts = [
            fir(lambda t, b=b: carried_ref[c, b, pl.ds(t, 8, stride=2 * STEPS2), :], STEPS2, CPAD) for b in range(3)
        ]
        high, low = split_columns(parts)
        ends, ends_low = high[:, :256], low[:, :256]
        both = jnp.concatenate([high[:, 256:], low[:, 256:]], axis=1)
        own = dot(ends, w_ref[0]) + dot(ends, w_ref[1]) + dot(ends_low, w_ref[0])
        own = own + dot(both, w_ref[2]) + dot(high[:, 256:], w_ref[3, :128, :])
        edge = dot(ends, w_ref[4]) + dot(both, w_ref[5])
        edge = edge[:, :128] + edge[:, 128:] + dot(ends_low, w_ref[4, :, :128])
        own_left = own[:, :128] + part_ref[c, 0]
        own_right = own[:, 128:] + part_ref[c, 1]
        for q in range(STEPS2):
            rows = pl.ds(q, 8, stride=STEPS2)
            linear_ref[c, 0, rows, :] = own_left[8 * q : 8 * q + 8]
            linear_ref[c, 1, rows, :] = own_right[8 * q : 8 * q + 8]
            linear_ref[c, 2, rows, :] = edge[8 * q : 8 * q + 8]
        return carry

    for c in range(4):
        reduce_two(c, 0)

    def finish_two(row, n, mask, out_row):
        rows = pl.ds(row, n)
        for b in range(3):
            linear = []
            for c in range(4):
                value = linear_ref[c, b, rows, :]
                if b == 2:
                    value = value * edge_mask
                if mask is not None:
                    value = value * mask
                linear.append(value)
            shown, carried = finish(linear)
            for c in range(4):
                if b < 2 and out_row is not None:
                    two_ref[c, pl.ds(out_row, n), 128 * b : 128 * b + 128] = shown[c]
                carried2_ref[c, b, rows, :] = carried[c]

    finish_two(0, 8, has_above, None)

    def body_two(i, carry):
        out_row = pl.multiple_of(16 * i, 16)
        finish_two(out_row + 8, 16, None, out_row)
        return carry

    lax.fori_loop(0, 16, body_two, 0)
    finish_two(264, 8, has_below, None)
    two_copy = pltpu.make_async_copy(two_ref, two_out, sem.at[4])
    two_copy.start()

    def reduce_three(c, carry):
        parts = [
            fir(lambda t, b=b: carried2_ref[c, b, pl.ds(t, 8, stride=2 * STEPS3), :], STEPS3, 8) for b in range(3)
        ]
        high, low = split_columns(parts)
        both = jnp.concatenate([high[:, 256:], low[:, 256:]], axis=1)
        total = dot(high[:, :256], w_ref[6]) + dot(both, w_ref[7])
        total = total[:, :128] + total[:, 128:] + dot(low[:, :256], w_ref[6, :, :128])
        for q in range(STEPS3):
            linear_ref[c, 0, pl.ds(q, 8, stride=STEPS3), :] = total[8 * q : 8 * q + 8]
        return carry

    for c in range(4):
        reduce_three(c, 0)
    for row in range(0, 128, 16):
        shown, _ = finish([linear_ref[c, 0, row : row + 16, :] for c in range(4)])
        for c in range(4):
            three_stage[c, row : row + 16, :] = shown[c]
    three_copy = pltpu.make_async_copy(three_stage, three_out, sem.at[5])
    three_copy.start()
    for pair in copies:
        for copy in pair:
            copy.wait()
    two_copy.wait()
    three_copy.wait()


VMEM = pl.BlockSpec(memory_space=pltpu.VMEM)
HBM = pl.BlockSpec(memory_space=pltpu.HBM)
ANY = pl.BlockSpec(memory_space=pl.ANY)
F32 = jnp.float32
BF16 = jnp.bfloat16


def params(mib):
    return pltpu.CompilerParams(vmem_limit_bytes=mib << 20)


def shifted(value, axis, steps):
    count = lax.axis_size(axis)
    pairs = [(i, i + steps) for i in range(count) if 0 <= i + steps < count]
    return lax.ppermute(value, axis, pairs)


def per_device(tiles, slot_tile):
    shape = jax.ShapeDtypeStruct
    band_shape = pltpu.VMEM((4, 5, TOP, 128), F32)
    pack_shape = pltpu.VMEM((3, PACK, 128), F32)
    in_hbm = lambda value: pltpu.with_memory_space_constraint(value, pltpu.HBM)
    weights, patch = in_hbm(jnp.asarray(tile_weights())), in_hbm(jnp.asarray(opacity_patch()))
    data, slots = in_hbm(tiles[0]), in_hbm(slot_tile)
    scratch = [
        pltpu.VMEM((8, 3, 2, TILE + 2 * XPAD, 128), F32),
        pltpu.VMEM((2, 3, PATCH, 256), BF16),
        pltpu.VMEM((3, 256, 256), BF16),
        pltpu.VMEM((3, PATCH, 128), F32),
        pltpu.SMEM((1, SLOTS), jnp.int32),
        pltpu.SMEM((SLOTS,), jnp.int32),
        pltpu.SemaphoreType.DMA((8, 2)),
        pltpu.SemaphoreType.DMA((3,)),
    ]
    outer, up, down = pl.pallas_call(
        outer_kernel,
        name="outer",
        out_shape=(pltpu.VMEM((4, 5, ROWS, 128), F32), band_shape, band_shape),
        in_specs=[HBM] * 4,
        out_specs=(VMEM, VMEM, VMEM),
        scratch_shapes=scratch,
        compiler_params=params(30),
    )(slots, data, weights, patch)
    below = shifted(up, "row", -1)
    above = shifted(down, "row", 1)
    inner = pl.pallas_call(
        inner_kernel,
        name="inner",
        out_shape=pltpu.VMEM((4, 5, INNER, 128), F32),
        in_specs=[HBM] * 4,
        out_specs=VMEM,
        scratch_shapes=scratch,
        cost_estimate=pl.CostEstimate(flops=4_000_000_000, bytes_accessed=4_000_000, transcendentals=0),
        compiler_params=params(30),
    )(slots, data, weights, patch)
    to_left, to_right, top, bottom = pl.pallas_call(
        pack_kernel,
        name="pack",
        out_shape=(pack_shape, pack_shape, band_shape, band_shape),
        in_specs=[VMEM, VMEM, ANY, ANY],
        out_specs=(VMEM,) * 4,
        scratch_shapes=[pltpu.VMEM((2, 4, 5, TOP, 128), F32), pltpu.SemaphoreType.DMA((2,))],
        compiler_params=params(20),
    )(outer, inner, above, below)
    from_right = shifted(to_left, "col", -1)
    from_left = shifted(to_right, "col", 1)
    middle, rest = level_two_weights()
    level_one, part, table = pl.pallas_call(
        middle_kernel,
        name="middle",
        out_shape=(
            shape((4, 512, 512), F32),
            pltpu.VMEM((4, 2, ROWS2, 128), F32),
            pltpu.VMEM((2, PATCH, 128), F32),
        ),
        in_specs=[VMEM] * 4 + [HBM] * 2,
        out_specs=(HBM, VMEM, VMEM),
        scratch_shapes=[
            pltpu.VMEM((4, 2, CROWS, 128), F32),
            pltpu.VMEM((4, 512, 256), F32),
            pltpu.VMEM((2, 256, 256), BF16),
            pltpu.SemaphoreType.DMA((4,)),
        ],
        cost_estimate=pl.CostEstimate(flops=4_000_000_000, bytes_accessed=4_000_000, transcendentals=0),
        compiler_params=params(30),
    )(outer, inner, top, bottom, in_hbm(jnp.asarray(middle)), in_hbm(jnp.asarray(band_opacity())))
    return pl.pallas_call(
        levels_kernel,
        name="levels",
        out_shape=(shape((4, 512, 512), F32), shape((4, 256, 256), F32), shape((4, 128, 128), F32)),
        in_specs=[VMEM] * 8 + [HBM] * 2,
        out_specs=(HBM, HBM, HBM),
        scratch_shapes=[
            pltpu.VMEM((2, 4, ROWS, 128), F32),
            pltpu.VMEM((4, 3, CROWS, 128), F32),
            pltpu.VMEM((4, 3, ROWS2, 128), F32),
            pltpu.VMEM((4, 3, ROWS2 + 16, 128), F32),
            pltpu.VMEM((2, 4, 512, 128), F32),
            pltpu.VMEM((4, 256, 256), F32),
            pltpu.VMEM((4, 128, 128), F32),
            pltpu.VMEM((8, 256, 256), BF16),
            pltpu.SemaphoreType.DMA((7,)),
        ],
        input_output_aliases={9: 0},
        compiler_params=params(30),
    )(outer, inner, top, bottom, from_left, from_right, part, table, in_hbm(jnp.asarray(rest)), level_one)


def solution(mesh):
    placed = (P("row", "col", None, None, None), P("row", "col"))
    return jax.shard_map(
        per_device,
        mesh=mesh,
        in_specs=placed,
        out_specs=(P(None, "row", "col"), P(None, "row", "col"), P(None, "row", "col")),
        check_vma=False,
    )
```

```python
import jax
import jax.numpy as jnp
import numpy as np
from jax import lax
from jax.experimental import pallas as pl
from jax.experimental.pallas import tpu as pltpu
from jax.sharding import PartitionSpec as P

BR = 4
BC = 4
SLOTS = 12
TILE = 256
WEIGHT_FLOOR = 0.25

ROWS = 544
INNER = 288
SURE = 4
QUOTA = 8
PATCH = 144
TOP = 24
BAND = 18
GROUPS = 7
PACK = 80
FLAG_ROW = 64
FLAG_LANE = 108
XPAD = 24
CPAD = 8
CROWS = 560
ROWS2 = 272


def lanczos(t):
    return np.where(np.abs(t) < 3.0, np.sinc(t) * np.sinc(t / 3.0), 0.0)


SUPPORT = lanczos((np.arange(-5, 7) - 0.5) / 2.0)
NORM = SUPPORT.sum()
TAPS = [float(np.float32(v / NORM)) for v in SUPPORT[5::-1]]


def taper(d):
    return (lanczos((d - 0.5) / 2.0) / NORM).astype(np.float32)


def split(matrix):
    high = matrix.astype(jnp.bfloat16)
    low = (matrix - high.astype(np.float32)).astype(jnp.bfloat16)
    return high, low


def tile_weights():
    x = np.arange(TILE)[:, None]
    lane = np.arange(128)[None, :]
    main = taper(x - 2 * lane)
    spill = np.where(lane < 8, taper(x - 2 * (lane + 128)), np.where(lane >= 120, taper(x - 2 * (lane - 128)), 0.0))
    spill = spill.astype(np.float32)
    mh, ml = split(main)
    sh, sl = split(spill)
    return np.stack([np.concatenate(pair, axis=1) for pair in ((mh, ml), (mh, sh), (sh, sl))])


def opacity_patch():
    x = np.arange(TILE)[None, :]
    rows = taper(x - 2 * np.arange(-8, PATCH - 8)[:, None]).sum(axis=1, dtype=np.float64)
    main = taper(x - 2 * np.arange(128)[:, None]).sum(axis=1, dtype=np.float64)
    lane = np.arange(128)
    right = taper(x - 2 * (lane[:, None] + 128)).sum(axis=1, dtype=np.float64)
    left = taper(x - 2 * (lane[:, None] - 128)).sum(axis=1, dtype=np.float64)
    cols = np.stack([main, np.where(lane >= 64, left, 0.0), np.where(lane < 64, right, 0.0)])
    return (cols[:, None, :] * rows[None, :, None]).astype(np.float32)


def band_opacity():
    main, left, right = opacity_patch()
    lane = np.arange(128)
    from_left = np.where(lane >= 113, main, np.where(lane < 3, right, 0.0))
    from_right = np.where(lane < 15, main, np.where(lane >= 125, left, 0.0))
    return np.stack([from_left, from_right]).astype(np.float32)


def wide_weights(own):
    edge = np.arange(128)
    cols_in = np.concatenate([np.arange(own), np.where(edge < 64, own + edge, edge - 128)])[:, None]
    cols_own = np.arange(own // 2)[None, :]
    cols_edge = np.where(edge < 64, own // 2 + edge, edge - 128)[None, :]
    return taper(cols_in - 2 * cols_own), taper(cols_in - 2 * cols_edge)


def level_two_weights():
    oh, ol = split(wide_weights(512)[0])
    eh, el = split(wide_weights(512)[1])
    th, tl = split(wide_weights(256)[0])
    zero = np.zeros((128, 128), eh.dtype)
    ends = lambda m: np.concatenate([m[:128], m[384:512]])
    beside = lambda *parts: np.concatenate(parts, axis=1)
    rest = [
        ends(oh),
        ends(ol),
        np.concatenate([oh[512:], oh[512:]]),
        np.concatenate([ol[512:], ol[512:]]),
        beside(ends(eh), ends(el)),
        np.concatenate([beside(eh[512:], el[512:]), beside(eh[512:], zero)]),
        beside(th[:256], tl[:256]),
        np.concatenate([beside(th[256:], tl[256:]), beside(th[256:], zero)]),
    ]
    return np.stack([oh[128:384], ol[128:384]]), np.stack(rest)


def fir(load, count, row0):
    rows = {}

    def at(t):
        if t not in rows:
            rows[t] = load(t)
        return rows[t]

    results = []
    for q in range(count):
        total = None
        for k, weight in enumerate(TAPS):
            term = (at(row0 + 2 * q - k) + at(row0 + 2 * q + 1 + k)) * weight
            total = term if total is None else total + term
        results.append(total)
    return results


def halves(value):
    high = value.astype(jnp.bfloat16)
    return high, (value - high.astype(jnp.float32)).astype(jnp.bfloat16)


def split_columns(parts):
    count = len(parts[0])
    highs, lows = [], []
    for q in range(0, count, 2):
        rows = [jnp.concatenate([part[p] for part in parts], axis=1) for p in range(q, min(q + 2, count))]
        high, low = halves(jnp.concatenate(rows, axis=0))
        highs.append(high)
        lows.append(low)
    return jnp.concatenate(highs, axis=0), jnp.concatenate(lows, axis=0)


def dot(left, right):
    return jnp.dot(left, right, preferred_element_type=jnp.float32)


def add_tiles(slot_hbm, tiles_ref, weight_ref, patch_ref, canvas_ref, x_ref, v_ref, w_ref, p_ref, slot_ref, list_ref, sem, wsem, outer):
    def copies(s, i):
        return [
            pltpu.make_async_copy(
                tiles_ref.at[s, :, :, pl.ds(128 * b, 128)], x_ref.at[i, :, b, pl.ds(XPAD, TILE), :], sem.at[i, b]
            )
            for b in range(2)
        ]

    loads = [pltpu.make_async_copy(weight_ref, w_ref, wsem.at[0]), pltpu.make_async_copy(patch_ref, p_ref, wsem.at[1])]
    slots = pltpu.make_async_copy(slot_hbm, slot_ref, wsem.at[2])
    slots.start()
    if outer:
        for s in range(SURE):
            list_ref[s] = s
            for copy in copies(s, s):
                copy.start()
    for copy in loads:
        copy.start()
    zero_pad = jnp.zeros((XPAD, 128), jnp.float32)

    def clear_pad(i, carry):
        for c in range(3):
            for b in range(2):
                x_ref[i, c, b, 0:XPAD, :] = zero_pad
                x_ref[i, c, b, XPAD + TILE : 2 * XPAD + TILE, :] = zero_pad
        return carry

    lax.fori_loop(0, x_ref.shape[0], clear_pad, 0)
    clear_canvas(canvas_ref, ROWS if outer else INNER)
    slots.wait()
    count = jnp.int32(SURE if outer else 0)
    places = [slot_ref[0, s] for s in range(SLOTS)]
    at_edge = [(place >= 0) & (((place >> 2) == 0) | ((place >> 2) == BR - 1)) for place in places]
    in_middle = [((place >> 2) == 1) | ((place >> 2) == 2) for place in places]
    edges = jnp.int32(0)
    for flag in at_edge[SURE:]:
        edges = edges + flag.astype(jnp.int32)
    spare = QUOTA - SURE - edges

    def take(s, wanted, count):
        @pl.when(wanted)
        def _():
            list_ref[count] = s
            for copy in copies(s, count):
                copy.start()

        return count + wanted.astype(jnp.int32)

    if outer:
        for s in range(SURE, SLOTS):
            count = take(s, at_edge[s], count)
    seen = jnp.int32(0)
    for s in range(SURE, SLOTS):
        wanted = in_middle[s] & ((seen < spare) if outer else (seen >= spare))
        count = take(s, wanted, count)
        seen = seen + in_middle[s].astype(jnp.int32)

    for copy in loads:
        copy.wait()

    lane = lax.broadcasted_iota(jnp.int32, (1, 128), 1)
    is_left = lane >= 64
    steps = PATCH // 8

    def arrive(i):
        for copy in copies(list_ref[i], i):
            copy.wait()

    def vertical(i):
        for c in range(3):
            parts = [
                fir(lambda t, b=b: x_ref[i, c, b, pl.ds(t, 8, stride=2 * steps), :], steps, XPAD - 16) for b in range(2)
            ]
            v_ref[0, c], v_ref[1, c] = split_columns(parts)

    def horizontal(i):
        place = slot_ref[0, list_ref[i]]
        tile_row = place >> 2
        tile_col = place & 3
        blocks = (tile_col, jnp.where(tile_col == 0, 4, tile_col - 1), tile_col + 1)
        row0 = pl.multiple_of(tile_row * 128 + (8 if outer else -120), 8)

        def add(c, rows, values):
            olds = [[canvas_ref[c, block, r, :] for r in rows] for block in blocks]
            for block, old, new in zip(blocks, olds, values):
                for r, first, second in zip(rows, old, new):
                    canvas_ref[c, block, r, :] = first + second

        for r in range(0, PATCH, 48):
            values = [[p_ref[k, r + t : r + t + 8, :] for t in range(0, 48, 8)] for k in range(3)]
            add(3, [pl.ds(row0 + r + t, 8) for t in range(0, 48, 8)], values)
        for c in range(3):
            first = dot(v_ref[0, c], w_ref[0])
            second = dot(v_ref[1, c], w_ref[1])
            third = dot(v_ref[0, c], w_ref[2])
            main = first[:, :128] + first[:, 128:] + second[:, :128]
            spill = second[:, 128:] + third[:, :128] + third[:, 128:]
            for q0 in range(0, steps, 6):
                mains = [main[8 * q : 8 * q + 8] for q in range(q0, q0 + 6)]
                spills = [spill[8 * q : 8 * q + 8] for q in range(q0, q0 + 6)]
                values = (mains, [jnp.where(is_left, v, 0.0) for v in spills], [jnp.where(is_left, 0.0, v) for v in spills])
                add(c, [pl.ds(row0 + q, 8, stride=steps) for q in range(q0, q0 + 6)], values)

    @pl.when(count > 0)
    def _():
        arrive(0)
        vertical(0)

        def step(i, carry):
            arrive(i)
            horizontal(i - 1)
            vertical(i)
            return carry

        lax.fori_loop(1, count, step, 0)
        horizontal(count - 1)


def clear_canvas(canvas_ref, count):
    zero_rows = jnp.zeros((count // 2, 128), jnp.float32)

    def clear(i, carry):
        c = i // 5
        b = i % 5
        canvas_ref[c, b, 0 : count // 2, :] = zero_rows
        canvas_ref[c, b, count // 2 : count, :] = zero_rows
        return carry

    lax.fori_loop(0, 20, clear, 0)


def outer_kernel(slot_ref, tiles_ref, weight_ref, patch_ref, canvas_ref, up_ref, down_ref, *scratch):
    add_tiles(slot_ref, tiles_ref, weight_ref, patch_ref, canvas_ref, *scratch, True)
    for c in range(4):
        for b in range(5):
            up_ref[c, b] = canvas_ref[c, b, 8:32, :]
            down_ref[c, b] = canvas_ref[c, b, 512:536, :]


def inner_kernel(slot_ref, tiles_ref, weight_ref, patch_ref, canvas_ref, *scratch):
    add_tiles(slot_ref, tiles_ref, weight_ref, patch_ref, canvas_ref, *scratch, False)


def canvas_rows(outer_ref, inner_ref, c, b, row, n, kind):
    value = outer_ref[c, b, pl.ds(row, n), :]
    return value + inner_ref[c, b, pl.ds(row - 128, n), :] if kind else value


KINDS = ((0, 128, 0), (128, 416, 1), (416, ROWS, 0))


def pack_kernel(outer_ref, inner_ref, above_any, below_any, left_ref, right_ref, top_ref, bottom_ref, band_ref, sem):
    bands = [pltpu.make_async_copy(ref, band_ref.at[k], sem.at[k]) for k, ref in enumerate((above_any, below_any))]
    for copy in bands:
        copy.start()
    lane = lax.broadcasted_iota(jnp.int32, (1, 128), 1)
    is_left = lane >= 64

    def rows_of(c, b, start):
        stop = min(start + PACK, ROWS)
        pieces = []
        for low, high, kind in KINDS:
            first, last = max(low, start), min(high, stop)
            if first < last:
                pieces.append(canvas_rows(outer_ref, inner_ref, c, b, first, last - first, kind))
        value = jnp.concatenate(pieces, axis=0) if len(pieces) > 1 else pieces[0]
        if start == 0:
            value = jnp.concatenate([top_ref[c, b], value[TOP:]], axis=0)
        if stop == ROWS:
            value = jnp.concatenate([value[:-TOP], bottom_ref[c, b]], axis=0)
        return value

    def packed(c, block, first, groups, start):
        for g in groups:
            edge, own = rows_of(c, 4, g * PACK), rows_of(c, block, g * PACK)
            band = jnp.where(is_left, edge, own) if block == 0 else jnp.where(is_left, own, edge)
            band = pltpu.roll(band, (first + BAND * g) % 128, 1)
            if start is None:
                start = band
                continue
            rows = band.shape[0]
            mask = (lane >= BAND * g) & (lane < BAND * (g + 1))
            head = jnp.where(mask, band, start[:rows])
            start = head if rows == PACK else jnp.concatenate([head, start[rows:]], axis=0)
        return start

    sides = ((left_ref, 0, 3), (right_ref, 3, 15))
    for c in range(3):
        for out_ref, block, first in sides:
            out_ref[c] = packed(c, block, first, range(1, GROUPS - 1), None)
    for copy in bands:
        copy.wait()
    for c in range(4):
        for b in range(5):
            top_ref[c, b] = outer_ref[c, b, 0:TOP, :] + band_ref[0, c, b]
            bottom_ref[c, b] = outer_ref[c, b, ROWS - TOP : ROWS, :] + band_ref[1, c, b]
    for c in range(3):
        for out_ref, block, first in sides:
            out_ref[c] = packed(c, block, first, (0, GROUPS - 1), out_ref[c])
    for out_ref, block, _ in sides:
        shown = [top_ref[3, block, 6:7, :]]
        for start in (76, 204, 332, 460):
            shown.append(canvas_rows(outer_ref, inner_ref, 3, block, start, 1, 128 <= start < 416))
        shown.append(bottom_ref[3, block, 16:17, :])
        for i, value in enumerate(shown):
            row = slice(FLAG_ROW + i, FLAG_ROW + i + 1)
            out_ref[0, row, :] = jnp.where(lane >= FLAG_LANE, value, out_ref[0, row, :])


def finish(linear):
    weight = linear[3]
    scale = 1.0 / jnp.maximum(weight, WEIGHT_FLOOR)
    opacity = jnp.clip(weight, 0.0, 1.0)
    colour = [linear[c] * scale for c in range(3)]
    return colour + [opacity], [value * opacity for value in colour] + [opacity]


def neighbours():
    row, col = lax.axis_index("row"), lax.axis_index("col")
    found = (row > 0, row < lax.axis_size("row") - 1, col > 0, col < lax.axis_size("col") - 1)
    return [jnp.where(flag, 1.0, 0.0).astype(jnp.float32) for flag in found]


def level_one_rows(top_ref, bottom_ref, finish_one, copies):
    has_above, has_below, _, _ = neighbours()

    def run(low, high, kind):
        def body(i, carry):
            row = pl.multiple_of(low + 16 * i, 16)
            finish_one(row, 16, None, 0, None, row - 16, kind)
            return carry

        lax.fori_loop(0, (high - low) // 16, body, 0)

    finish_one(0, 16, top_ref, 0, has_above, None, 0)
    finish_one(16, 8, top_ref, 16, None, 0, 0)
    finish_one(24, 8, None, 0, None, 8, 0)
    run(32, 128, 0)
    run(128, 272, 1)
    for copy in copies[0]:
        copy.start()
    run(272, 416, 1)
    run(416, 512, 0)
    finish_one(512, 8, None, 0, None, 496, 0)
    finish_one(520, 8, bottom_ref, 0, None, 504, 0)
    for copy in copies[1]:
        copy.start()
    finish_one(528, 16, bottom_ref, 8, has_below, None, 0)


def clear_carried(carried_ref, blocks):
    zero_pad = jnp.zeros((CPAD, 128), jnp.float32)
    for c in range(4):
        for b in range(blocks):
            carried_ref[c, b, 0:CPAD, :] = zero_pad
            carried_ref[c, b, CPAD + ROWS : CROWS, :] = zero_pad


STEPS2 = ROWS2 // 8
STEPS3 = 17


def middle_kernel(outer_ref, inner_ref, top_ref, bottom_ref, own_hbm, table_hbm, one_out, part_ref, table_ref, carried_ref, one_ref, own_ref, sem):
    load = pltpu.make_async_copy(own_hbm, own_ref, sem.at[2])
    load.start()
    table_load = pltpu.make_async_copy(table_hbm, table_ref, sem.at[3])
    table_load.start()
    clear_carried(carried_ref, 2)

    def finish_one(row, n, band, band_row, mask, out_row, kind):
        for b in range(2):
            linear = []
            for c in range(4):
                if band is None:
                    value = canvas_rows(outer_ref, inner_ref, c, b + 1, row, n, kind)
                else:
                    value = band[c, b + 1, pl.ds(band_row, n), :]
                if mask is not None:
                    value = value * mask
                linear.append(value)
            shown, carried = finish(linear)
            for c in range(4):
                if out_row is not None:
                    one_ref[c, pl.ds(out_row, n), 128 * b : 128 * b + 128] = shown[c]
                carried_ref[c, b, pl.ds(row + CPAD, n), :] = carried[c]

    copies = [
        [
            pltpu.make_async_copy(
                one_ref.at[:, pl.ds(256 * q, 256), :], one_out.at[:, pl.ds(256 * q, 256), pl.ds(128, 256)], sem.at[q]
            )
        ]
        for q in range(2)
    ]
    level_one_rows(top_ref, bottom_ref, finish_one, copies)
    load.wait()
    table_load.wait()

    def reduce_two(c, carry):
        parts = [
            fir(lambda t, b=b: carried_ref[c, b, pl.ds(t, 8, stride=2 * STEPS2), :], STEPS2, CPAD) for b in range(2)
        ]
        high, low = split_columns(parts)
        own = dot(high, own_ref[0]) + dot(high, own_ref[1]) + dot(low, own_ref[0])
        part_ref[c, 0] = own[:, :128]
        part_ref[c, 1] = own[:, 128:]
        return carry

    for c in range(4):
        reduce_two(c, 0)
    for pair in copies:
        for copy in pair:
            copy.wait()


def levels_kernel(
    outer_ref, inner_ref, top_ref, bottom_ref, from_left_ref, from_right_ref, part_ref, table_ref, own_hbm, one_in,
    one_out, two_out, three_out,
    add_ref, carried_ref, linear_ref, carried2_ref, one_ref, two_ref, three_stage, w_ref, sem,
):
    load = pltpu.make_async_copy(own_hbm, w_ref, sem.at[6])
    load.start()
    has_above, has_below, has_left, has_right = neighbours()
    lane = lax.broadcasted_iota(jnp.int32, (1, 128), 1)
    is_left = lane >= 64
    edge_mask = jnp.where(is_left, has_left, has_right)
    clear_carried(carried_ref, 3)
    for c in range(4):
        for b in range(3):
            carried2_ref[c, b, ROWS2 : ROWS2 + 16, :] = jnp.zeros((16, 128), jnp.float32)

    from_left_lanes = (lane >= 113) | (lane < 3)
    from_right_lanes = (lane >= 125) | (lane < 15)
    for c in range(3):
        for side, ref, first, lanes in ((0, from_left_ref, 15, from_left_lanes), (1, from_right_ref, 3, from_right_lanes)):
            for g in range(GROUPS):
                start, stop = g * PACK, min(g * PACK + PACK, ROWS)
                band = pltpu.roll(ref[c, 0 : stop - start, :], (-first - BAND * g) % 128, 1)
                add_ref[side, c, start:stop, :] = jnp.where(lanes, band, 0.0)

    for side, ref in ((0, from_left_ref), (1, from_right_ref)):
        flags = [
            jnp.where(ref[0, FLAG_ROW + i : FLAG_ROW + i + 1, FLAG_LANE : FLAG_LANE + 1] > 0.5, 1.0, 0.0) for i in range(6)
        ]
        flags = [jnp.broadcast_to(flag, (8, 128)) for flag in flags]
        for start in range(0, ROWS, 8):
            total = None
            for i in range(6):
                row = start - 128 * (i - 1) - 8
                if 0 <= row < PATCH:
                    term = table_ref[side, row : row + 8, :] * flags[i]
                    total = term if total is None else total + term
            add_ref[side, 3, start : start + 8, :] = total

    def finish_one(row, n, band, band_row, mask, out_row, kind):
        rows = pl.ds(row, n)
        for b, block in enumerate((0, 3, 4)):
            linear = []
            for c in range(4):
                if band is None:
                    value = canvas_rows(outer_ref, inner_ref, c, block, row, n, kind)
                else:
                    value = band[c, block, pl.ds(band_row, n), :]
                if b == 0:
                    value = value + jnp.where(is_left, 0.0, add_ref[0, c, rows, :])
                if b == 1:
                    value = value + jnp.where(is_left, add_ref[1, c, rows, :], 0.0)
                if b == 2:
                    value = value + jnp.where(is_left, add_ref[0, c, rows, :], add_ref[1, c, rows, :])
                    value = value * edge_mask
                if mask is not None:
                    value = value * mask
                linear.append(value)
            shown, carried = finish(linear)
            for c in range(4):
                if b < 2 and out_row is not None:
                    one_ref[b, c, pl.ds(out_row, n), :] = shown[c]
                carried_ref[c, b, pl.ds(row + CPAD, n), :] = carried[c]

    copies = [
        [
            pltpu.make_async_copy(
                one_ref.at[b, :, pl.ds(256 * q, 256), :],
                one_out.at[:, pl.ds(256 * q, 256), pl.ds(384 * b, 128)],
                sem.at[2 * q + b],
            )
            for b in range(2)
        ]
        for q in range(2)
    ]
    level_one_rows(top_ref, bottom_ref, finish_one, copies)
    load.wait()

    def reduce_two(c, carry):
        parts = [
            fir(lambda t, b=b: carried_ref[c, b, pl.ds(t, 8, stride=2 * STEPS2), :], STEPS2, CPAD) for b in range(3)
        ]
        high, low = split_columns(parts)
        ends, ends_low = high[:, :256], low[:, :256]
        both = jnp.concatenate([high[:, 256:], low[:, 256:]], axis=1)
        own = dot(ends, w_ref[0]) + dot(ends, w_ref[1]) + dot(ends_low, w_ref[0])
        own = own + dot(both, w_ref[2]) + dot(high[:, 256:], w_ref[3, :128, :])
        edge = dot(ends, w_ref[4]) + dot(both, w_ref[5])
        edge = edge[:, :128] + edge[:, 128:] + dot(ends_low, w_ref[4, :, :128])
        own_left = own[:, :128] + part_ref[c, 0]
        own_right = own[:, 128:] + part_ref[c, 1]
        for q in range(STEPS2):
            rows = pl.ds(q, 8, stride=STEPS2)
            linear_ref[c, 0, rows, :] = own_left[8 * q : 8 * q + 8]
            linear_ref[c, 1, rows, :] = own_right[8 * q : 8 * q + 8]
            linear_ref[c, 2, rows, :] = edge[8 * q : 8 * q + 8]
        return carry

    for c in range(4):
        reduce_two(c, 0)

    def finish_two(row, n, mask, out_row):
        rows = pl.ds(row, n)
        for b in range(3):
            linear = []
            for c in range(4):
                value = linear_ref[c, b, rows, :]
                if b == 2:
                    value = value * edge_mask
                if mask is not None:
                    value = value * mask
                linear.append(value)
            shown, carried = finish(linear)
            for c in range(4):
                if b < 2 and out_row is not None:
                    two_ref[c, pl.ds(out_row, n), 128 * b : 128 * b + 128] = shown[c]
                carried2_ref[c, b, rows, :] = carried[c]

    finish_two(0, 8, has_above, None)

    def body_two(i, carry):
        out_row = pl.multiple_of(16 * i, 16)
        finish_two(out_row + 8, 16, None, out_row)
        return carry

    lax.fori_loop(0, 16, body_two, 0)
    finish_two(264, 8, has_below, None)
    two_copy = pltpu.make_async_copy(two_ref, two_out, sem.at[4])
    two_copy.start()

    def reduce_three(c, carry):
        parts = [
            fir(lambda t, b=b: carried2_ref[c, b, pl.ds(t, 8, stride=2 * STEPS3), :], STEPS3, 8) for b in range(3)
        ]
        high, low = split_columns(parts)
        both = jnp.concatenate([high[:, 256:], low[:, 256:]], axis=1)
        total = dot(high[:, :256], w_ref[6]) + dot(both, w_ref[7])
        total = total[:, :128] + total[:, 128:] + dot(low[:, :256], w_ref[6, :, :128])
        for q in range(STEPS3):
            linear_ref[c, 0, pl.ds(q, 8, stride=STEPS3), :] = total[8 * q : 8 * q + 8]
        return carry

    for c in range(4):
        reduce_three(c, 0)
    for row in range(0, 128, 16):
        shown, _ = finish([linear_ref[c, 0, row : row + 16, :] for c in range(4)])
        for c in range(4):
            three_stage[c, row : row + 16, :] = shown[c]
    three_copy = pltpu.make_async_copy(three_stage, three_out, sem.at[5])
    three_copy.start()
    for pair in copies:
        for copy in pair:
            copy.wait()
    two_copy.wait()
    three_copy.wait()


VMEM = pl.BlockSpec(memory_space=pltpu.VMEM)
HBM = pl.BlockSpec(memory_space=pltpu.HBM)
ANY = pl.BlockSpec(memory_space=pl.ANY)
F32 = jnp.float32
BF16 = jnp.bfloat16


def params(mib):
    return pltpu.CompilerParams(vmem_limit_bytes=mib << 20)


def shifted(value, axis, steps):
    count = lax.axis_size(axis)
    pairs = [(i, i + steps) for i in range(count) if 0 <= i + steps < count]
    return lax.ppermute(value, axis, pairs)


def per_device(tiles, slot_tile):
    shape = jax.ShapeDtypeStruct
    band_shape = pltpu.VMEM((4, 5, TOP, 128), F32)
    pack_shape = pltpu.VMEM((3, PACK, 128), F32)
    in_hbm = lambda value: pltpu.with_memory_space_constraint(value, pltpu.HBM)
    weights, patch = in_hbm(jnp.asarray(tile_weights())), in_hbm(jnp.asarray(opacity_patch()))
    data, slots = in_hbm(tiles[0]), in_hbm(slot_tile)
    scratch = lambda held: [
        pltpu.VMEM((held, 3, 2, TILE + 2 * XPAD, 128), F32),
        pltpu.VMEM((2, 3, PATCH, 256), BF16),
        pltpu.VMEM((3, 256, 256), BF16),
        pltpu.VMEM((3, PATCH, 128), F32),
        pltpu.SMEM((1, SLOTS), jnp.int32),
        pltpu.SMEM((SLOTS,), jnp.int32),
        pltpu.SemaphoreType.DMA((held, 2)),
        pltpu.SemaphoreType.DMA((3,)),
    ]
    outer, up, down = pl.pallas_call(
        outer_kernel,
        name="outer",
        out_shape=(pltpu.VMEM((4, 5, ROWS, 128), F32), band_shape, band_shape),
        in_specs=[HBM] * 4,
        out_specs=(VMEM, VMEM, VMEM),
        scratch_shapes=scratch(SLOTS),
        compiler_params=params(30),
    )(slots, data, weights, patch)
    below = shifted(up, "row", -1)
    above = shifted(down, "row", 1)
    inner = pl.pallas_call(
        inner_kernel,
        name="inner",
        out_shape=pltpu.VMEM((4, 5, INNER, 128), F32),
        in_specs=[HBM] * 4,
        out_specs=VMEM,
        scratch_shapes=scratch(QUOTA - SURE),
        cost_estimate=pl.CostEstimate(flops=4_000_000_000, bytes_accessed=4_000_000, transcendentals=0),
        compiler_params=params(30),
    )(slots, data, weights, patch)
    to_left, to_right, top, bottom = pl.pallas_call(
        pack_kernel,
        name="pack",
        out_shape=(pack_shape, pack_shape, band_shape, band_shape),
        in_specs=[VMEM, VMEM, ANY, ANY],
        out_specs=(VMEM,) * 4,
        scratch_shapes=[pltpu.VMEM((2, 4, 5, TOP, 128), F32), pltpu.SemaphoreType.DMA((2,))],
        compiler_params=params(20),
    )(outer, inner, above, below)
    from_right = shifted(to_left, "col", -1)
    from_left = shifted(to_right, "col", 1)
    middle, rest = level_two_weights()
    level_one, part, table = pl.pallas_call(
        middle_kernel,
        name="middle",
        out_shape=(
            shape((4, 512, 512), F32),
            pltpu.VMEM((4, 2, ROWS2, 128), F32),
            pltpu.VMEM((2, PATCH, 128), F32),
        ),
        in_specs=[VMEM] * 4 + [HBM] * 2,
        out_specs=(HBM, VMEM, VMEM),
        scratch_shapes=[
            pltpu.VMEM((4, 2, CROWS, 128), F32),
            pltpu.VMEM((4, 512, 256), F32),
            pltpu.VMEM((2, 256, 256), BF16),
            pltpu.SemaphoreType.DMA((4,)),
        ],
        cost_estimate=pl.CostEstimate(flops=4_000_000_000, bytes_accessed=4_000_000, transcendentals=0),
        compiler_params=params(30),
    )(outer, inner, top, bottom, in_hbm(jnp.asarray(middle)), in_hbm(jnp.asarray(band_opacity())))
    return pl.pallas_call(
        levels_kernel,
        name="levels",
        out_shape=(shape((4, 512, 512), F32), shape((4, 256, 256), F32), shape((4, 128, 128), F32)),
        in_specs=[VMEM] * 8 + [HBM] * 2,
        out_specs=(HBM, HBM, HBM),
        scratch_shapes=[
            pltpu.VMEM((2, 4, ROWS, 128), F32),
            pltpu.VMEM((4, 3, CROWS, 128), F32),
            pltpu.VMEM((4, 3, ROWS2, 128), F32),
            pltpu.VMEM((4, 3, ROWS2 + 16, 128), F32),
            pltpu.VMEM((2, 4, 512, 128), F32),
            pltpu.VMEM((4, 256, 256), F32),
            pltpu.VMEM((4, 128, 128), F32),
            pltpu.VMEM((8, 256, 256), BF16),
            pltpu.SemaphoreType.DMA((7,)),
        ],
        input_output_aliases={9: 0},
        compiler_params=params(30),
    )(outer, inner, top, bottom, from_left, from_right, part, table, in_hbm(jnp.asarray(rest)), level_one)


def solution(mesh):
    placed = (P("row", "col", None, None, None), P("row", "col"))
    return jax.shard_map(
        per_device,
        mesh=mesh,
        in_specs=placed,
        out_specs=(P(None, "row", "col"), P(None, "row", "col"), P(None, "row", "col")),
        check_vma=False,
    )
```

```python
import jax
import jax.numpy as jnp
import numpy as np
from jax import lax
from jax.experimental import pallas as pl
from jax.experimental.pallas import tpu as pltpu
from jax.sharding import PartitionSpec as P

BR = 4
BC = 4
SLOTS = 12
TILE = 256
WEIGHT_FLOOR = 0.25

ROWS = 544
INNER = 288
SURE = 4
QUOTA = 6
PATCH = 144
TOP = 24
BAND = 18
GROUPS = 7
PACK = 80
FLAG_ROW = 64
FLAG_LANE = 108
XPAD = 24
CPAD = 8
CROWS = 560
ROWS2 = 272


def lanczos(t):
    return np.where(np.abs(t) < 3.0, np.sinc(t) * np.sinc(t / 3.0), 0.0)


SUPPORT = lanczos((np.arange(-5, 7) - 0.5) / 2.0)
NORM = SUPPORT.sum()
TAPS = [float(np.float32(v / NORM)) for v in SUPPORT[5::-1]]


def taper(d):
    return (lanczos((d - 0.5) / 2.0) / NORM).astype(np.float32)


def split(matrix):
    high = matrix.astype(jnp.bfloat16)
    low = (matrix - high.astype(np.float32)).astype(jnp.bfloat16)
    return high, low


def tile_weights():
    x = np.arange(TILE)[:, None]
    lane = np.arange(128)[None, :]
    main = taper(x - 2 * lane)
    spill = np.where(lane < 8, taper(x - 2 * (lane + 128)), np.where(lane >= 120, taper(x - 2 * (lane - 128)), 0.0))
    spill = spill.astype(np.float32)
    mh, ml = split(main)
    sh, sl = split(spill)
    return np.stack([np.concatenate(pair, axis=1) for pair in ((mh, ml), (mh, sh), (sh, sl))])


def opacity_patch():
    x = np.arange(TILE)[None, :]
    rows = taper(x - 2 * np.arange(-8, PATCH - 8)[:, None]).sum(axis=1, dtype=np.float64)
    main = taper(x - 2 * np.arange(128)[:, None]).sum(axis=1, dtype=np.float64)
    lane = np.arange(128)
    right = taper(x - 2 * (lane[:, None] + 128)).sum(axis=1, dtype=np.float64)
    left = taper(x - 2 * (lane[:, None] - 128)).sum(axis=1, dtype=np.float64)
    cols = np.stack([main, np.where(lane >= 64, left, 0.0), np.where(lane < 64, right, 0.0)])
    return (cols[:, None, :] * rows[None, :, None]).astype(np.float32)


def band_opacity():
    main, left, right = opacity_patch()
    lane = np.arange(128)
    from_left = np.where(lane >= 113, main, np.where(lane < 3, right, 0.0))
    from_right = np.where(lane < 15, main, np.where(lane >= 125, left, 0.0))
    return np.stack([from_left, from_right]).astype(np.float32)


def wide_weights(own):
    edge = np.arange(128)
    cols_in = np.concatenate([np.arange(own), np.where(edge < 64, own + edge, edge - 128)])[:, None]
    cols_own = np.arange(own // 2)[None, :]
    cols_edge = np.where(edge < 64, own // 2 + edge, edge - 128)[None, :]
    return taper(cols_in - 2 * cols_own), taper(cols_in - 2 * cols_edge)


def level_two_weights():
    oh, ol = split(wide_weights(512)[0])
    eh, el = split(wide_weights(512)[1])
    th, tl = split(wide_weights(256)[0])
    zero = np.zeros((128, 128), eh.dtype)
    ends = lambda m: np.concatenate([m[:128], m[384:512]])
    beside = lambda *parts: np.concatenate(parts, axis=1)
    rest = [
        ends(oh),
        ends(ol),
        np.concatenate([oh[512:], oh[512:]]),
        np.concatenate([ol[512:], ol[512:]]),
        beside(ends(eh), ends(el)),
        np.concatenate([beside(eh[512:], el[512:]), beside(eh[512:], zero)]),
        beside(th[:256], tl[:256]),
        np.concatenate([beside(th[256:], tl[256:]), beside(th[256:], zero)]),
    ]
    return np.stack([oh[128:384], ol[128:384]]), np.stack(rest)


def fir(load, count, row0):
    rows = {}

    def at(t):
        if t not in rows:
            rows[t] = load(t)
        return rows[t]

    results = []
    for q in range(count):
        total = None
        for k, weight in enumerate(TAPS):
            term = (at(row0 + 2 * q - k) + at(row0 + 2 * q + 1 + k)) * weight
            total = term if total is None else total + term
        results.append(total)
    return results


def halves(value):
    high = value.astype(jnp.bfloat16)
    return high, (value - high.astype(jnp.float32)).astype(jnp.bfloat16)


def split_columns(parts):
    count = len(parts[0])
    highs, lows = [], []
    for q in range(0, count, 2):
        rows = [jnp.concatenate([part[p] for part in parts], axis=1) for p in range(q, min(q + 2, count))]
        high, low = halves(jnp.concatenate(rows, axis=0))
        highs.append(high)
        lows.append(low)
    return jnp.concatenate(highs, axis=0), jnp.concatenate(lows, axis=0)


def dot(left, right):
    return jnp.dot(left, right, preferred_element_type=jnp.float32)


def add_tiles(slot_hbm, tiles_ref, weight_ref, patch_ref, canvas_ref, x_ref, v_ref, w_ref, p_ref, slot_ref, list_ref, sem, wsem, outer):
    def copies(s, i):
        return [
            pltpu.make_async_copy(
                tiles_ref.at[s, :, :, pl.ds(128 * b, 128)], x_ref.at[i, :, b, pl.ds(XPAD, TILE), :], sem.at[i, b]
            )
            for b in range(2)
        ]

    loads = [pltpu.make_async_copy(weight_ref, w_ref, wsem.at[0]), pltpu.make_async_copy(patch_ref, p_ref, wsem.at[1])]
    slots = pltpu.make_async_copy(slot_hbm, slot_ref, wsem.at[2])
    slots.start()
    if outer:
        for s in range(SURE):
            list_ref[s] = s
            for copy in copies(s, s):
                copy.start()
    for copy in loads:
        copy.start()
    zero_pad = jnp.zeros((XPAD, 128), jnp.float32)

    def clear_pad(i, carry):
        for c in range(3):
            for b in range(2):
                x_ref[i, c, b, 0:XPAD, :] = zero_pad
                x_ref[i, c, b, XPAD + TILE : 2 * XPAD + TILE, :] = zero_pad
        return carry

    lax.fori_loop(0, x_ref.shape[0], clear_pad, 0)
    clear_canvas(canvas_ref, ROWS if outer else INNER)
    slots.wait()
    count = jnp.int32(SURE if outer else 0)
    places = [slot_ref[0, s] for s in range(SLOTS)]
    at_edge = [(place >= 0) & (((place >> 2) == 0) | ((place >> 2) == BR - 1)) for place in places]
    in_middle = [((place >> 2) == 1) | ((place >> 2) == 2) for place in places]
    edges = jnp.int32(0)
    for flag in at_edge[SURE:]:
        edges = edges + flag.astype(jnp.int32)
    spare = QUOTA - SURE - edges

    def take(s, wanted, count):
        @pl.when(wanted)
        def _():
            list_ref[count] = s
            for copy in copies(s, count):
                copy.start()

        return count + wanted.astype(jnp.int32)

    if outer:
        for s in range(SURE, SLOTS):
            count = take(s, at_edge[s], count)
    seen = jnp.int32(0)
    for s in range(SURE, SLOTS):
        wanted = in_middle[s] & ((seen < spare) if outer else (seen >= spare))
        count = take(s, wanted, count)
        seen = seen + in_middle[s].astype(jnp.int32)

    for copy in loads:
        copy.wait()

    lane = lax.broadcasted_iota(jnp.int32, (1, 128), 1)
    is_left = lane >= 64
    steps = PATCH // 8

    def arrive(i):
        for copy in copies(list_ref[i], i):
            copy.wait()

    def vertical(i):
        for c in range(3):
            parts = [
                fir(lambda t, b=b: x_ref[i, c, b, pl.ds(t, 8, stride=2 * steps), :], steps, XPAD - 16) for b in range(2)
            ]
            v_ref[0, c], v_ref[1, c] = split_columns(parts)

    def horizontal(i):
        place = slot_ref[0, list_ref[i]]
        tile_row = place >> 2
        tile_col = place & 3
        blocks = (tile_col, jnp.where(tile_col == 0, 4, tile_col - 1), tile_col + 1)
        row0 = pl.multiple_of(tile_row * 128 + (8 if outer else -120), 8)

        def add(c, rows, values):
            olds = [[canvas_ref[c, block, r, :] for r in rows] for block in blocks]
            for block, old, new in zip(blocks, olds, values):
                for r, first, second in zip(rows, old, new):
                    canvas_ref[c, block, r, :] = first + second

        for r in range(0, PATCH, 48):
            values = [[p_ref[k, r + t : r + t + 8, :] for t in range(0, 48, 8)] for k in range(3)]
            add(3, [pl.ds(row0 + r + t, 8) for t in range(0, 48, 8)], values)
        for c in range(3):
            first = dot(v_ref[0, c], w_ref[0])
            second = dot(v_ref[1, c], w_ref[1])
            third = dot(v_ref[0, c], w_ref[2])
            main = first[:, :128] + first[:, 128:] + second[:, :128]
            spill = second[:, 128:] + third[:, :128] + third[:, 128:]
            for q0 in range(0, steps, 6):
                mains = [main[8 * q : 8 * q + 8] for q in range(q0, q0 + 6)]
                spills = [spill[8 * q : 8 * q + 8] for q in range(q0, q0 + 6)]
                values = (mains, [jnp.where(is_left, v, 0.0) for v in spills], [jnp.where(is_left, 0.0, v) for v in spills])
                add(c, [pl.ds(row0 + q, 8, stride=steps) for q in range(q0, q0 + 6)], values)

    @pl.when(count > 0)
    def _():
        arrive(0)
        vertical(0)

        def step(i, carry):
            arrive(i)
            horizontal(i - 1)
            vertical(i)
            return carry

        lax.fori_loop(1, count, step, 0)
        horizontal(count - 1)


def clear_canvas(canvas_ref, count):
    zero_rows = jnp.zeros((count // 2, 128), jnp.float32)

    def clear(i, carry):
        c = i // 5
        b = i % 5
        canvas_ref[c, b, 0 : count // 2, :] = zero_rows
        canvas_ref[c, b, count // 2 : count, :] = zero_rows
        return carry

    lax.fori_loop(0, 20, clear, 0)


def outer_kernel(slot_ref, tiles_ref, weight_ref, patch_ref, canvas_ref, up_ref, down_ref, *scratch):
    add_tiles(slot_ref, tiles_ref, weight_ref, patch_ref, canvas_ref, *scratch, True)
    for c in range(4):
        for b in range(5):
            up_ref[c, b] = canvas_ref[c, b, 8:32, :]
            down_ref[c, b] = canvas_ref[c, b, 512:536, :]


def inner_kernel(slot_ref, tiles_ref, weight_ref, patch_ref, canvas_ref, *scratch):
    add_tiles(slot_ref, tiles_ref, weight_ref, patch_ref, canvas_ref, *scratch, False)


def canvas_rows(outer_ref, inner_ref, c, b, row, n, kind):
    value = outer_ref[c, b, pl.ds(row, n), :]
    return value + inner_ref[c, b, pl.ds(row - 128, n), :] if kind else value


KINDS = ((0, 128, 0), (128, 416, 1), (416, ROWS, 0))


def pack_kernel(outer_ref, inner_ref, above_any, below_any, left_ref, right_ref, top_ref, bottom_ref, band_ref, sem):
    bands = [pltpu.make_async_copy(ref, band_ref.at[k], sem.at[k]) for k, ref in enumerate((above_any, below_any))]
    for copy in bands:
        copy.start()
    lane = lax.broadcasted_iota(jnp.int32, (1, 128), 1)
    is_left = lane >= 64

    def rows_of(c, b, start):
        stop = min(start + PACK, ROWS)
        pieces = []
        for low, high, kind in KINDS:
            first, last = max(low, start), min(high, stop)
            if first < last:
                pieces.append(canvas_rows(outer_ref, inner_ref, c, b, first, last - first, kind))
        value = jnp.concatenate(pieces, axis=0) if len(pieces) > 1 else pieces[0]
        if start == 0:
            value = jnp.concatenate([top_ref[c, b], value[TOP:]], axis=0)
        if stop == ROWS:
            value = jnp.concatenate([value[:-TOP], bottom_ref[c, b]], axis=0)
        return value

    def packed(c, block, first, groups, start):
        for g in groups:
            edge, own = rows_of(c, 4, g * PACK), rows_of(c, block, g * PACK)
            band = jnp.where(is_left, edge, own) if block == 0 else jnp.where(is_left, own, edge)
            band = pltpu.roll(band, (first + BAND * g) % 128, 1)
            if start is None:
                start = band
                continue
            rows = band.shape[0]
            mask = (lane >= BAND * g) & (lane < BAND * (g + 1))
            head = jnp.where(mask, band, start[:rows])
            start = head if rows == PACK else jnp.concatenate([head, start[rows:]], axis=0)
        return start

    sides = ((left_ref, 0, 3), (right_ref, 3, 15))
    for c in range(3):
        for out_ref, block, first in sides:
            out_ref[c] = packed(c, block, first, range(1, GROUPS - 1), None)
    for copy in bands:
        copy.wait()
    for c in range(4):
        for b in range(5):
            top_ref[c, b] = outer_ref[c, b, 0:TOP, :] + band_ref[0, c, b]
            bottom_ref[c, b] = outer_ref[c, b, ROWS - TOP : ROWS, :] + band_ref[1, c, b]
    for c in range(3):
        for out_ref, block, first in sides:
            out_ref[c] = packed(c, block, first, (0, GROUPS - 1), out_ref[c])
    for out_ref, block, _ in sides:
        shown = [top_ref[3, block, 6:7, :]]
        for start in (76, 204, 332, 460):
            shown.append(canvas_rows(outer_ref, inner_ref, 3, block, start, 1, 128 <= start < 416))
        shown.append(bottom_ref[3, block, 16:17, :])
        for i, value in enumerate(shown):
            row = slice(FLAG_ROW + i, FLAG_ROW + i + 1)
            out_ref[0, row, :] = jnp.where(lane >= FLAG_LANE, value, out_ref[0, row, :])


def finish(linear):
    weight = linear[3]
    scale = 1.0 / jnp.maximum(weight, WEIGHT_FLOOR)
    opacity = jnp.clip(weight, 0.0, 1.0)
    colour = [linear[c] * scale for c in range(3)]
    return colour + [opacity], [value * opacity for value in colour] + [opacity]


def neighbours():
    row, col = lax.axis_index("row"), lax.axis_index("col")
    found = (row > 0, row < lax.axis_size("row") - 1, col > 0, col < lax.axis_size("col") - 1)
    return [jnp.where(flag, 1.0, 0.0).astype(jnp.float32) for flag in found]


def level_one_rows(top_ref, bottom_ref, finish_one, copies):
    has_above, has_below, _, _ = neighbours()

    def run(low, high, kind):
        def body(i, carry):
            row = pl.multiple_of(low + 16 * i, 16)
            finish_one(row, 16, None, 0, None, row - 16, kind)
            return carry

        lax.fori_loop(0, (high - low) // 16, body, 0)

    finish_one(0, 16, top_ref, 0, has_above, None, 0)
    finish_one(16, 8, top_ref, 16, None, 0, 0)
    finish_one(24, 8, None, 0, None, 8, 0)
    run(32, 128, 0)
    run(128, 272, 1)
    for copy in copies[0]:
        copy.start()
    run(272, 416, 1)
    run(416, 512, 0)
    finish_one(512, 8, None, 0, None, 496, 0)
    finish_one(520, 8, bottom_ref, 0, None, 504, 0)
    for copy in copies[1]:
        copy.start()
    finish_one(528, 16, bottom_ref, 8, has_below, None, 0)


def clear_carried(carried_ref, blocks):
    zero_pad = jnp.zeros((CPAD, 128), jnp.float32)
    for c in range(4):
        for b in range(blocks):
            carried_ref[c, b, 0:CPAD, :] = zero_pad
            carried_ref[c, b, CPAD + ROWS : CROWS, :] = zero_pad


STEPS2 = ROWS2 // 8
STEPS3 = 17


def middle_kernel(outer_ref, inner_ref, top_ref, bottom_ref, own_hbm, table_hbm, one_out, part_ref, table_ref, carried_ref, one_ref, own_ref, sem):
    load = pltpu.make_async_copy(own_hbm, own_ref, sem.at[2])
    load.start()
    table_load = pltpu.make_async_copy(table_hbm, table_ref, sem.at[3])
    table_load.start()
    clear_carried(carried_ref, 2)

    def finish_one(row, n, band, band_row, mask, out_row, kind):
        for b in range(2):
            linear = []
            for c in range(4):
                if band is None:
                    value = canvas_rows(outer_ref, inner_ref, c, b + 1, row, n, kind)
                else:
                    value = band[c, b + 1, pl.ds(band_row, n), :]
                if mask is not None:
                    value = value * mask
                linear.append(value)
            shown, carried = finish(linear)
            for c in range(4):
                if out_row is not None:
                    one_ref[c, pl.ds(out_row, n), 128 * b : 128 * b + 128] = shown[c]
                carried_ref[c, b, pl.ds(row + CPAD, n), :] = carried[c]

    copies = [
        [
            pltpu.make_async_copy(
                one_ref.at[:, pl.ds(256 * q, 256), :], one_out.at[:, pl.ds(256 * q, 256), pl.ds(128, 256)], sem.at[q]
            )
        ]
        for q in range(2)
    ]
    level_one_rows(top_ref, bottom_ref, finish_one, copies)
    load.wait()
    table_load.wait()

    def reduce_two(c, carry):
        parts = [
            fir(lambda t, b=b: carried_ref[c, b, pl.ds(t, 8, stride=2 * STEPS2), :], STEPS2, CPAD) for b in range(2)
        ]
        high, low = split_columns(parts)
        own = dot(high, own_ref[0]) + dot(high, own_ref[1]) + dot(low, own_ref[0])
        part_ref[c, 0] = own[:, :128]
        part_ref[c, 1] = own[:, 128:]
        return carry

    for c in range(4):
        reduce_two(c, 0)
    for pair in copies:
        for copy in pair:
            copy.wait()


def levels_kernel(
    outer_ref, inner_ref, top_ref, bottom_ref, from_left_ref, from_right_ref, part_ref, table_ref, own_hbm, one_in,
    one_out, two_out, three_out,
    add_ref, carried_ref, linear_ref, carried2_ref, one_ref, two_ref, three_stage, w_ref, sem,
):
    load = pltpu.make_async_copy(own_hbm, w_ref, sem.at[6])
    load.start()
    has_above, has_below, has_left, has_right = neighbours()
    lane = lax.broadcasted_iota(jnp.int32, (1, 128), 1)
    is_left = lane >= 64
    edge_mask = jnp.where(is_left, has_left, has_right)
    clear_carried(carried_ref, 3)
    for c in range(4):
        for b in range(3):
            carried2_ref[c, b, ROWS2 : ROWS2 + 16, :] = jnp.zeros((16, 128), jnp.float32)

    from_left_lanes = (lane >= 113) | (lane < 3)
    from_right_lanes = (lane >= 125) | (lane < 15)
    for c in range(3):
        for side, ref, first, lanes in ((0, from_left_ref, 15, from_left_lanes), (1, from_right_ref, 3, from_right_lanes)):
            for g in range(GROUPS):
                start, stop = g * PACK, min(g * PACK + PACK, ROWS)
                band = pltpu.roll(ref[c, 0 : stop - start, :], (-first - BAND * g) % 128, 1)
                add_ref[side, c, start:stop, :] = jnp.where(lanes, band, 0.0)

    for side, ref in ((0, from_left_ref), (1, from_right_ref)):
        flags = [
            jnp.where(ref[0, FLAG_ROW + i : FLAG_ROW + i + 1, FLAG_LANE : FLAG_LANE + 1] > 0.5, 1.0, 0.0) for i in range(6)
        ]
        flags = [jnp.broadcast_to(flag, (8, 128)) for flag in flags]
        for start in range(0, ROWS, 8):
            total = None
            for i in range(6):
                row = start - 128 * (i - 1) - 8
                if 0 <= row < PATCH:
                    term = table_ref[side, row : row + 8, :] * flags[i]
                    total = term if total is None else total + term
            add_ref[side, 3, start : start + 8, :] = total

    def finish_one(row, n, band, band_row, mask, out_row, kind):
        rows = pl.ds(row, n)
        for b, block in enumerate((0, 3, 4)):
            linear = []
            for c in range(4):
                if band is None:
                    value = canvas_rows(outer_ref, inner_ref, c, block, row, n, kind)
                else:
                    value = band[c, block, pl.ds(band_row, n), :]
                if b == 0:
                    value = value + jnp.where(is_left, 0.0, add_ref[0, c, rows, :])
                if b == 1:
                    value = value + jnp.where(is_left, add_ref[1, c, rows, :], 0.0)
                if b == 2:
                    value = value + jnp.where(is_left, add_ref[0, c, rows, :], add_ref[1, c, rows, :])
                    value = value * edge_mask
                if mask is not None:
                    value = value * mask
                linear.append(value)
            shown, carried = finish(linear)
            for c in range(4):
                if b < 2 and out_row is not None:
                    one_ref[b, c, pl.ds(out_row, n), :] = shown[c]
                carried_ref[c, b, pl.ds(row + CPAD, n), :] = carried[c]

    copies = [
        [
            pltpu.make_async_copy(
                one_ref.at[b, :, pl.ds(256 * q, 256), :],
                one_out.at[:, pl.ds(256 * q, 256), pl.ds(384 * b, 128)],
                sem.at[2 * q + b],
            )
            for b in range(2)
        ]
        for q in range(2)
    ]
    level_one_rows(top_ref, bottom_ref, finish_one, copies)
    load.wait()

    def reduce_two(c, carry):
        parts = [
            fir(lambda t, b=b: carried_ref[c, b, pl.ds(t, 8, stride=2 * STEPS2), :], STEPS2, CPAD) for b in range(3)
        ]
        high, low = split_columns(parts)
        ends, ends_low = high[:, :256], low[:, :256]
        both = jnp.concatenate([high[:, 256:], low[:, 256:]], axis=1)
        own = dot(ends, w_ref[0]) + dot(ends, w_ref[1]) + dot(ends_low, w_ref[0])
        own = own + dot(both, w_ref[2]) + dot(high[:, 256:], w_ref[3, :128, :])
        edge = dot(ends, w_ref[4]) + dot(both, w_ref[5])
        edge = edge[:, :128] + edge[:, 128:] + dot(ends_low, w_ref[4, :, :128])
        own_left = own[:, :128] + part_ref[c, 0]
        own_right = own[:, 128:] + part_ref[c, 1]
        for q in range(STEPS2):
            rows = pl.ds(q, 8, stride=STEPS2)
            linear_ref[c, 0, rows, :] = own_left[8 * q : 8 * q + 8]
            linear_ref[c, 1, rows, :] = own_right[8 * q : 8 * q + 8]
            linear_ref[c, 2, rows, :] = edge[8 * q : 8 * q + 8]
        return carry

    for c in range(4):
        reduce_two(c, 0)

    def finish_two(row, n, mask, out_row):
        rows = pl.ds(row, n)
        for b in range(3):
            linear = []
            for c in range(4):
                value = linear_ref[c, b, rows, :]
                if b == 2:
                    value = value * edge_mask
                if mask is not None:
                    value = value * mask
                linear.append(value)
            shown, carried = finish(linear)
            for c in range(4):
                if b < 2 and out_row is not None:
                    two_ref[c, pl.ds(out_row, n), 128 * b : 128 * b + 128] = shown[c]
                carried2_ref[c, b, rows, :] = carried[c]

    finish_two(0, 8, has_above, None)

    def body_two(i, carry):
        out_row = pl.multiple_of(16 * i, 16)
        finish_two(out_row + 8, 16, None, out_row)
        return carry

    lax.fori_loop(0, 16, body_two, 0)
    finish_two(264, 8, has_below, None)
    two_copy = pltpu.make_async_copy(two_ref, two_out, sem.at[4])
    two_copy.start()

    def reduce_three(c, carry):
        parts = [
            fir(lambda t, b=b: carried2_ref[c, b, pl.ds(t, 8, stride=2 * STEPS3), :], STEPS3, 8) for b in range(3)
        ]
        high, low = split_columns(parts)
        both = jnp.concatenate([high[:, 256:], low[:, 256:]], axis=1)
        total = dot(high[:, :256], w_ref[6]) + dot(both, w_ref[7])
        total = total[:, :128] + total[:, 128:] + dot(low[:, :256], w_ref[6, :, :128])
        for q in range(STEPS3):
            linear_ref[c, 0, pl.ds(q, 8, stride=STEPS3), :] = total[8 * q : 8 * q + 8]
        return carry

    for c in range(4):
        reduce_three(c, 0)
    for row in range(0, 128, 16):
        shown, _ = finish([linear_ref[c, 0, row : row + 16, :] for c in range(4)])
        for c in range(4):
            three_stage[c, row : row + 16, :] = shown[c]
    three_copy = pltpu.make_async_copy(three_stage, three_out, sem.at[5])
    three_copy.start()
    for pair in copies:
        for copy in pair:
            copy.wait()
    two_copy.wait()
    three_copy.wait()


VMEM = pl.BlockSpec(memory_space=pltpu.VMEM)
HBM = pl.BlockSpec(memory_space=pltpu.HBM)
ANY = pl.BlockSpec(memory_space=pl.ANY)
F32 = jnp.float32
BF16 = jnp.bfloat16


def params(mib):
    return pltpu.CompilerParams(vmem_limit_bytes=mib << 20)


def shifted(value, axis, steps):
    count = lax.axis_size(axis)
    pairs = [(i, i + steps) for i in range(count) if 0 <= i + steps < count]
    return lax.ppermute(value, axis, pairs)


def per_device(tiles, slot_tile):
    shape = jax.ShapeDtypeStruct
    band_shape = pltpu.VMEM((4, 5, TOP, 128), F32)
    pack_shape = pltpu.VMEM((3, PACK, 128), F32)
    in_hbm = lambda value: pltpu.with_memory_space_constraint(value, pltpu.HBM)
    weights, patch = in_hbm(jnp.asarray(tile_weights())), in_hbm(jnp.asarray(opacity_patch()))
    data, slots = in_hbm(tiles[0]), in_hbm(slot_tile)
    scratch = lambda held: [
        pltpu.VMEM((held, 3, 2, TILE + 2 * XPAD, 128), F32),
        pltpu.VMEM((2, 3, PATCH, 256), BF16),
        pltpu.VMEM((3, 256, 256), BF16),
        pltpu.VMEM((3, PATCH, 128), F32),
        pltpu.SMEM((1, SLOTS), jnp.int32),
        pltpu.SMEM((SLOTS,), jnp.int32),
        pltpu.SemaphoreType.DMA((held, 2)),
        pltpu.SemaphoreType.DMA((3,)),
    ]
    outer, up, down = pl.pallas_call(
        outer_kernel,
        name="outer",
        out_shape=(pltpu.VMEM((4, 5, ROWS, 128), F32), band_shape, band_shape),
        in_specs=[HBM] * 4,
        out_specs=(VMEM, VMEM, VMEM),
        scratch_shapes=scratch(SLOTS),
        compiler_params=params(30),
    )(slots, data, weights, patch)
    below = shifted(up, "row", -1)
    above = shifted(down, "row", 1)
    inner = pl.pallas_call(
        inner_kernel,
        name="inner",
        out_shape=pltpu.VMEM((4, 5, INNER, 128), F32),
        in_specs=[HBM] * 4,
        out_specs=VMEM,
        scratch_shapes=scratch(SLOTS - QUOTA),
        cost_estimate=pl.CostEstimate(flops=4_000_000_000, bytes_accessed=4_000_000, transcendentals=0),
        compiler_params=params(30),
    )(slots, data, weights, patch)
    to_left, to_right, top, bottom = pl.pallas_call(
        pack_kernel,
        name="pack",
        out_shape=(pack_shape, pack_shape, band_shape, band_shape),
        in_specs=[VMEM, VMEM, ANY, ANY],
        out_specs=(VMEM,) * 4,
        scratch_shapes=[pltpu.VMEM((2, 4, 5, TOP, 128), F32), pltpu.SemaphoreType.DMA((2,))],
        compiler_params=params(20),
    )(outer, inner, above, below)
    from_right = shifted(to_left, "col", -1)
    from_left = shifted(to_right, "col", 1)
    middle, rest = level_two_weights()
    level_one, part, table = pl.pallas_call(
        middle_kernel,
        name="middle",
        out_shape=(
            shape((4, 512, 512), F32),
            pltpu.VMEM((4, 2, ROWS2, 128), F32),
            pltpu.VMEM((2, PATCH, 128), F32),
        ),
        in_specs=[VMEM] * 4 + [HBM] * 2,
        out_specs=(HBM, VMEM, VMEM),
        scratch_shapes=[
            pltpu.VMEM((4, 2, CROWS, 128), F32),
            pltpu.VMEM((4, 512, 256), F32),
            pltpu.VMEM((2, 256, 256), BF16),
            pltpu.SemaphoreType.DMA((4,)),
        ],
        cost_estimate=pl.CostEstimate(flops=4_000_000_000, bytes_accessed=4_000_000, transcendentals=0),
        compiler_params=params(30),
    )(outer, inner, top, bottom, in_hbm(jnp.asarray(middle)), in_hbm(jnp.asarray(band_opacity())))
    return pl.pallas_call(
        levels_kernel,
        name="levels",
        out_shape=(shape((4, 512, 512), F32), shape((4, 256, 256), F32), shape((4, 128, 128), F32)),
        in_specs=[VMEM] * 8 + [HBM] * 2,
        out_specs=(HBM, HBM, HBM),
        scratch_shapes=[
            pltpu.VMEM((2, 4, ROWS, 128), F32),
            pltpu.VMEM((4, 3, CROWS, 128), F32),
            pltpu.VMEM((4, 3, ROWS2, 128), F32),
            pltpu.VMEM((4, 3, ROWS2 + 16, 128), F32),
            pltpu.VMEM((2, 4, 512, 128), F32),
            pltpu.VMEM((4, 256, 256), F32),
            pltpu.VMEM((4, 128, 128), F32),
            pltpu.VMEM((8, 256, 256), BF16),
            pltpu.SemaphoreType.DMA((7,)),
        ],
        input_output_aliases={9: 0},
        compiler_params=params(30),
    )(outer, inner, top, bottom, from_left, from_right, part, table, in_hbm(jnp.asarray(rest)), level_one)


def solution(mesh):
    placed = (P("row", "col", None, None, None), P("row", "col"))
    return jax.shard_map(
        per_device,
        mesh=mesh,
        in_specs=placed,
        out_specs=(P(None, "row", "col"), P(None, "row", "col"), P(None, "row", "col")),
        check_vma=False,
    )
```
